32 devices in a mesh: pair: 4 (over x, core), ep: 8 (over z, y).
Axes of the slice: x: 2, y: 2, z: 4, core: 2. Of those that a mesh axis runs over, the one named last changes fastest.
Arguments:
- tokens: bfloat16 [8192, 4096], P(('pair', 'ep')), may hold values from -6 to 6
- expert_of: int32 [8192, 1], P(('pair', 'ep')), may hold values from 0 to 31, as said below
- w_gate: bfloat16 [32, 4096, 768], P(('pair', 'ep')), may hold values from -0.09375 to 0.09375
- w_up: bfloat16 [32, 4096, 768], P(('pair', 'ep')), may hold values from -0.09375 to 0.09375
- w_down: bfloat16 [32, 768, 4096], P(('pair', 'ep')), may hold values from -0.21875 to 0.21875
Outputs:
- mixed: bfloat16 [8192, 4096], P(('pair', 'ep'))
The draws below stay inside these ranges and needn't reach their ends.
Inputs may be any that keep to these rules, and one draw needn't show every extreme that they name: `expert_of`: the rows of one device (aligned blocks of 256 tokens) name no expert more than 12 times; in every draw one expert, drawn from the seed, is named exactly 12 times in every device's rows.
All inputs are finite; a program needn't handle non-finite values.
Results may differ from the reference program's by a relative error of at most 0.005.
Values may be sent and summed in bfloat16 or wider, within the bound.
A program may use at most 128 MiB of HBM per device.

```python
import jax
import jax.numpy as jnp
from jax import lax

D = 4096
FF = 768
TOK_DEV = 256
EXPERTS = 32
CAP = 12
TOKENS = 8192


def draw_expert_of(key, part):
    blocks = TOKENS // TOK_DEV
    hottest = jax.random.randint(jax.random.fold_in(key, 7), (), 0, EXPERTS).astype(jnp.int32)
    block_keys = jax.random.split(jax.random.fold_in(key, 11), blocks)

    def one_block(block_key):
        first_key, second_key = jax.random.split(block_key)
        others = jnp.repeat(jnp.arange(EXPERTS - 1, dtype=jnp.int32), CAP)
        others = jax.random.permutation(first_key, others)[:TOK_DEV - CAP]
        others = others + (others >= hottest).astype(jnp.int32)
        block_rows = jnp.concatenate([jnp.full((CAP,), hottest, jnp.int32), others])
        return jax.random.permutation(second_key, block_rows)
    return jax.vmap(one_block)(block_keys).reshape(TOKENS, 1).astype(jnp.int32)


def steps_of(stream_key, dims, shards, least, high):
    def one(dim, blocks):
        steps = jax.random.uniform(jax.random.fold_in(jax.random.fold_in(stream_key, 6), dim), (blocks,), jnp.float32, least / len(shards), high / len(shards))
        return jnp.repeat(jnp.exp(steps), dims[dim] // blocks).reshape((-1,) + (1,) * (len(dims) - dim - 1))

    level = one(*shards[0])
    for cut in shards[1:]:
        level = level * one(*cut)
    return level


def normal_values(stream_key, extent, scale, bound, cuts=(), kind=jnp.bfloat16):
    values = scale * jax.random.normal(stream_key, extent, jnp.float32)
    if cuts:
        values = values * steps_of(stream_key, extent, cuts, -0.22, 0.18)
    return jnp.clip(values, -bound, bound).astype(kind)


def setup_inputs(seed: int = 0) -> dict:
    keys = jax.random.split(jax.random.key(seed), 6)
    return {
        "tokens": normal_values(keys[0], (TOKENS, D), 1.0, 6.0, ((0, 32),)),
        "expert_of": draw_expert_of(jax.random.fold_in(keys[5], 71), 0),
        "w_gate": normal_values(keys[2], (EXPERTS, D, FF), D ** -0.5, 0.09375, ((0, 32),)),
        "w_up": normal_values(keys[3], (EXPERTS, D, FF), D ** -0.5, 0.09375, ((0, 32),)),
        "w_down": normal_values(keys[4], (EXPERTS, FF, D), FF ** -0.5, 0.21875, ((0, 32),)),
    }


def reference(tokens, expert_of, w_gate, w_up, w_down):
    routed = expert_of[:, 0].astype(jnp.int32)
    row_limit = EXPERTS * CAP
    sorted_rows = jnp.argsort(routed, stable=True).astype(jnp.int32)
    expert_load = jnp.sum((routed[:, None] == jnp.arange(EXPERTS, dtype=jnp.int32)[None, :]).astype(jnp.int32), axis=0).astype(jnp.int32)
    offsets = (jnp.cumsum(expert_load) - expert_load).astype(jnp.int32)
    padded_order = jnp.concatenate([sorted_rows, jnp.full((row_limit,), TOKENS, jnp.int32)])

    def per_expert(mixed_sofar, expert):
        picked = lax.dynamic_slice(padded_order, (offsets[expert].astype(jnp.int32),), (row_limit,))
        is_live = jnp.arange(row_limit, dtype=jnp.int32) < expert_load[expert]
        picked = jnp.where(is_live, picked, TOKENS).astype(jnp.int32)
        gathered = jnp.take(tokens, jnp.minimum(picked, TOKENS - 1), axis=0)
        gate_proj = jnp.dot(gathered, w_gate[expert], preferred_element_type=jnp.float32)
        up_proj = jnp.dot(gathered, w_up[expert], preferred_element_type=jnp.float32)
        hidden = (jax.nn.silu(gate_proj) * up_proj).astype(jnp.bfloat16)
        result = jnp.dot(hidden, w_down[expert], preferred_element_type=jnp.float32).astype(jnp.bfloat16)
        return mixed_sofar.at[picked].set(result, mode="drop"), None

    start = jnp.zeros((TOKENS, D), jnp.bfloat16)
    mixed, _ = lax.scan(per_expert, start, jnp.arange(EXPERTS, dtype=jnp.int32))
    return mixed
```

```python
import functools

import jax
import jax.numpy as jnp
from jax import lax
from jax.experimental import pallas as pl
from jax.experimental.pallas import tpu as pltpu
from jax.sharding import PartitionSpec as P

MESH = pl.DeviceIdType.MESH
TILE = 16
GROUP = 8


def dot(a, b):
    return jnp.dot(a, b, preferred_element_type=jnp.float32)


def exchange_ffn(
    pairs, eps, cap, row_keys, col_keys, tok_hbm, gate_hbm, up_hbm, down_hbm, head_ref, ends_ref,
    tok, outgoing, recv, result, returned, gate, up, down, hidden, rest,
    tok_sem, w_sem, local_sem, send1, recv1, send2, recv2,
):
    n = pairs * eps
    pair, ep = lax.axis_index("pair"), lax.axis_index("ep")
    tok_rows = tok.shape[0]
    width = recv.shape[2]
    tail = rest.shape[1]
    parts = cap // (TILE - cap)
    spare = TILE - cap
    rows = GROUP * TILE
    bf16 = jnp.bfloat16

    def shift(k):
        i = k // pairs
        de = (eps // 2 + ((i + 1) // 2) * (2 * ((i + 1) % 2) - 1) + eps) % eps
        return (k + 1) % pairs, de

    def target(k):
        dp, de = shift(k)
        return lax.rem(pair + dp, pairs), lax.rem(ep + de, eps)

    def origin(k):
        dp, de = shift(k)
        return lax.rem(pair + pairs - dp, pairs), lax.rem(ep + eps - de, eps)

    tok_load = pltpu.make_async_copy(tok_hbm, tok, tok_sem.at[0])
    tok_load.start()

    barrier = pltpu.get_barrier_semaphore()

    @pl.loop(0, n - 1)
    def _(k):
        p, e = target(k)
        pl.semaphore_signal(barrier, inc=1, device_id=(p, e), device_id_type=MESH)

    loads = [
        pltpu.make_async_copy(src.at[0], dst, w_sem.at[i])
        for i, (src, dst) in enumerate(((gate_hbm, gate), (up_hbm, up), (down_hbm, down)))
    ]
    for load in loads:
        load.start()

    def outbound(k):
        p, e = target(k)
        return pltpu.make_async_remote_copy(
            src_ref=outgoing.at[k],
            dst_ref=recv.at[k],
            send_sem=send1.at[k],
            recv_sem=recv1.at[k],
            device_id=(p, e),
            device_id_type=MESH,
        )

    def inbound(k):
        p, e = origin(k)
        return pltpu.make_async_remote_copy(
            src_ref=result.at[k],
            dst_ref=returned.at[k],
            send_sem=send2.at[k],
            recv_sem=recv2.at[k],
            device_id=(p, e),
            device_id_type=MESH,
        )

    def row_ids(first, shape, axis):
        at = lax.broadcasted_iota(jnp.int32, shape, axis)
        base = jnp.zeros(shape, jnp.int32)
        for i in range(GROUP):
            p, e = target(first + i)
            base = jnp.where(at // TILE == i, (p * eps + e) * TILE, base)
        return base + at % TILE

    def one_hot(mask):
        return mask.astype(jnp.float32).astype(bf16)

    def pack(first):
        ids = row_ids(first, (rows, tok_rows), 0)
        main = one_hot(row_keys[0:1, :] == ids)
        for j in range(parts):
            cols = pl.ds(j * tail, tail)
            ends = one_hot(row_keys[j + 1:j + 2, :] == ids)
            piece = dot(main, tok[:, cols]) + dot(ends, tok[:, width:])
            outgoing[pl.ds(first, GROUP), :, cols] = piece.astype(bf16).reshape(GROUP, TILE, tail)

    def unpack(first, start):
        ids = row_ids(first, (tok_rows, rows), 1)
        main = one_hot(col_keys[:, 0:1] == ids)
        ends = jnp.zeros((tok_rows, tail), jnp.float32)
        for j in range(parts):
            cols = pl.ds(j * tail, tail)
            piece = returned[pl.ds(first, GROUP), :, cols].reshape(rows, tail)
            head = dot(main, piece).astype(bf16)
            head_ref[:, cols] = head if start else head_ref[:, cols] + head
            ends = ends + dot(one_hot(col_keys[:, j + 1:j + 2] == ids), piece)
        ends = ends.astype(bf16)
        ends_ref[...] = ends if start else ends_ref[...] + ends

    def send(first):
        @pl.loop(0, GROUP)
        def _(i):
            @pl.when(first + i < n - 1)
            def _():
                outbound(first + i).start()

    tok_load.wait()
    pack(0)
    pl.semaphore_wait(barrier, n - 1)
    send(0)

    @pl.loop(1, n // GROUP)
    def _(g):
        pack(g * GROUP)
        send(g * GROUP)

    own = pltpu.make_async_copy(outgoing.at[n - 1], recv.at[n - 1], local_sem.at[0])
    own.start()
    for load in loads:
        load.wait()
    own.wait()

    r = lax.broadcasted_iota(jnp.int32, (rows, rows), 0)
    c = lax.broadcasted_iota(jnp.int32, (rows, rows), 1)
    same = (r // TILE) == (c // TILE)
    r, c = r % TILE, c % TILE

    def spreader(j):
        return one_hot(same & (r // spare == j) & (c == cap + r % spare))

    def folder(j):
        return one_hot(same & (r >= cap) & (c == spare * j + r - cap))

    body_row = (lax.broadcasted_iota(jnp.int32, (rows, 1), 0) % TILE) < cap
    step = 256

    @pl.loop(0, n // GROUP)
    def _(g):
        first = g * GROUP

        @pl.loop(0, GROUP)
        def _(i):
            @pl.when(first + i < n - 1)
            def _():
                outbound(first + i).wait_recv()

        block = recv.at[pl.ds(first, GROUP)]
        total = jnp.zeros((rows, tail), jnp.float32)
        for j in range(parts):
            piece = block[:, :, j * tail:(j + 1) * tail].reshape(rows, tail)
            total = total + dot(spreader(j), piece)
        rest[...] = total.astype(bf16)

        @pl.loop(0, hidden.shape[1] // step)
        def _(f):
            cols = pl.ds(pl.multiple_of(f * step, step), step)
            main = block[...].reshape(rows, width)
            g_out = dot(main, gate[:width, cols]) + dot(rest[...], gate[width:, cols])
            u_out = dot(main, up[:width, cols]) + dot(rest[...], up[width:, cols])
            hidden[:, cols] = (jax.nn.silu(g_out) * u_out).astype(bf16)

        rest[...] = dot(hidden[...], down[:, width:]).astype(bf16)
        for j in range(parts):
            cols = pl.ds(j * tail, tail)
            body = dot(hidden[...], down[:, cols])
            extra = dot(folder(j), rest[...])
            packed = jnp.where(body_row, body, extra).astype(bf16)
            result[pl.ds(first, GROUP), :, cols] = packed.reshape(GROUP, TILE, tail)

        @pl.loop(0, GROUP)
        def _(i):
            @pl.when(first + i < n - 1)
            def _():
                inbound(first + i).start()

    mine = pltpu.make_async_copy(result.at[n - 1], returned.at[n - 1], local_sem.at[1])
    mine.start()
    mine.wait()

    def collect(first):
        @pl.loop(0, GROUP)
        def _(i):
            @pl.when(first + i < n - 1)
            def _():
                inbound(first + i).wait_recv()

    collect(0)
    unpack(0, True)

    @pl.loop(1, n // GROUP)
    def _(g):
        collect(g * GROUP)
        unpack(g * GROUP, False)

    @pl.loop(0, n - 1)
    def _(k):
        outbound(k).wait_send()
        inbound(k).wait_send()


def fused(tokens, routed, slot, w_gate, w_up, w_down, pairs, eps, cap):
    n = pairs * eps
    tok_rows, depth = tokens.shape
    ff = w_gate.shape[2]
    spare = TILE - cap
    parts = cap // spare
    tail = depth * spare // TILE
    width = depth - tail

    rest_key = jnp.where(
        slot[None, :] // spare == jnp.arange(parts)[:, None],
        (routed * TILE + cap + slot % spare)[None, :],
        -1,
    )
    keys = jnp.concatenate([(routed * TILE + slot)[None, :], rest_key], axis=0)

    vmem = pl.BlockSpec(memory_space=pltpu.VMEM)
    hbm = pl.BlockSpec(memory_space=pl.ANY)
    bf16 = jnp.bfloat16
    parcels = pltpu.VMEM((n, TILE, width), bf16)
    head, ends = pl.pallas_call(
        functools.partial(exchange_ffn, pairs, eps, cap),
        out_shape=[
            jax.ShapeDtypeStruct((tok_rows, width), bf16),
            jax.ShapeDtypeStruct((tok_rows, tail), bf16),
        ],
        in_specs=[vmem, vmem, hbm, hbm, hbm, hbm],
        out_specs=[vmem, vmem],
        scratch_shapes=[
            pltpu.VMEM((tok_rows, depth), bf16),
            parcels,
            parcels,
            parcels,
            parcels,
            pltpu.VMEM((depth, ff), bf16),
            pltpu.VMEM((depth, ff), bf16),
            pltpu.VMEM((ff, depth), bf16),
            pltpu.VMEM((GROUP * TILE, ff), bf16),
            pltpu.VMEM((GROUP * TILE, tail), bf16),
            pltpu.SemaphoreType.DMA((1,)),
            pltpu.SemaphoreType.DMA((3,)),
            pltpu.SemaphoreType.DMA((2,)),
            pltpu.SemaphoreType.DMA((n,)),
            pltpu.SemaphoreType.DMA((n,)),
            pltpu.SemaphoreType.DMA((n,)),
            pltpu.SemaphoreType.DMA((n,)),
        ],
        compiler_params=pltpu.CompilerParams(
            collective_id=0, has_side_effects=True, vmem_limit_bytes=56 * 1024 * 1024
        ),
        name="exchange_ffn",
    )(keys, keys.T, tokens, w_gate, w_up, w_down)
    return jnp.concatenate([head, ends], axis=1)


def plain(tokens, routed, slot, w_gate, w_up, w_down, experts, capacity):
    position = routed * capacity + slot
    outgoing = (
        jnp.zeros((experts * capacity, tokens.shape[1]), jnp.bfloat16).at[position].set(tokens)
    )
    parcel = lax.all_to_all(
        outgoing.reshape(experts, capacity, outgoing.shape[1]),
        ("pair", "ep"), split_axis=0, concat_axis=0, tiled=True,
    )
    flat_rows = parcel.reshape(experts * capacity, parcel.shape[2])
    gate_proj = dot(flat_rows, w_gate[0])
    up_proj = dot(flat_rows, w_up[0])
    hidden = (jax.nn.silu(gate_proj) * up_proj).astype(jnp.bfloat16)
    result = dot(hidden, w_down[0]).astype(jnp.bfloat16)
    returned = lax.all_to_all(
        result.reshape(experts, capacity, result.shape[1]),
        ("pair", "ep"), split_axis=0, concat_axis=0, tiled=True,
    )
    return jnp.take(returned.reshape(experts * capacity, -1), position, axis=0)


BLOCK = 8


def near_ffn(
    pairs, eps, spill, keys_ref, tok_hbm, gate_hbm, up_hbm, down_hbm, out_hbm, flag_ref,
    tok, send_b, recv_b, res_b, ret_b, send_x, recv_x, res_x, ret_x, send_s, recv_s, res_s, ret_s,
    note, notes, gate, up, down, rows_x, hidden, total,
    tok_sem, w_sem, out_sem, ssem_b, rsem_b, ssem_x, rsem_x, ssem_s, rsem_s, ssem_n, rsem_n,
):
    n = pairs * eps
    near = n // 2
    line = eps // 2
    pair, ep = lax.axis_index("pair"), lax.axis_index("ep")
    side, spot = ep // line, ep % line
    tok_rows, depth = tok.shape
    mid = depth // 2
    ff = hidden.shape[1]
    extra = BLOCK // 2
    bf16, f32, i32 = jnp.bfloat16, jnp.float32, jnp.int32
    none = -4 * n * TILE
    wide = 512

    def peer(k, sign):
        j = k % near + 1
        p = lax.rem(pair + pairs + sign * (j // line % pairs), pairs)
        s = lax.rem(spot + line + sign * (j % line), line)
        return p, lax.rem(side + 1 - k // near, 2) * line + s

    tok_load = pltpu.make_async_copy(tok_hbm, tok, tok_sem.at[0])
    tok_load.start()
    barrier = pltpu.get_barrier_semaphore()

    @pl.loop(0, n - 1)
    def _(k):
        pl.semaphore_signal(barrier, inc=1, device_id=peer(k, 1), device_id_type=MESH)

    loads = [
        pltpu.make_async_copy(src.at[0], dst, w_sem.at[i])
        for i, (src, dst) in enumerate(((gate_hbm, gate), (up_hbm, up), (down_hbm, down)))
    ]
    for load in loads:
        load.start()

    def remote(src, dst, ssem, rsem, to):
        return pltpu.make_async_remote_copy(
            src_ref=src, dst_ref=dst, send_sem=ssem, recv_sem=rsem,
            device_id=to, device_id_type=MESH,
        )

    def out_b(k):
        return remote(send_b.at[k], recv_b.at[k], ssem_b.at[0, k], rsem_b.at[0, k], peer(k, 1))

    def back_b(k):
        return remote(res_b.at[k], ret_b.at[k], ssem_b.at[1, k], rsem_b.at[1, k], peer(k, -1))

    def out_x(k):
        return remote(
            send_x.at[k], recv_x.at[k], ssem_x.at[0, k], rsem_x.at[0, k], peer(k + near, 1)
        )

    def back_x(k):
        return remote(
            res_x.at[k], ret_x.at[k], ssem_x.at[1, k], rsem_x.at[1, k], peer(k + near, -1)
        )

    mirror = (pair, lax.rem(side + 1, 2) * line + spot)
    out_s = remote(send_s, recv_s, ssem_s.at[0], rsem_s.at[0], mirror)
    back_s = remote(res_s, ret_s, ssem_s.at[1], rsem_s.at[1], mirror)

    def tell(k):
        return remote(note, notes.at[k], ssem_n.at[k], rsem_n.at[k], peer(k, 1))

    def iota(shape, axis):
        return lax.broadcasted_iota(i32, shape, axis)

    def one_hot(mask):
        return jnp.where(mask, 1.0, 0.0).astype(bf16)

    expert = iota((n, 128), 0)
    order = jnp.zeros((n, 128), i32)
    for k in range(n):
        p, e = peer(k, 1) if k < n - 1 else (pair, ep)
        order = jnp.where(expert == p * eps + e, k, order)
    order = order.astype(f32)
    routed = keys_ref[0:1, :]
    chosen = jnp.where(iota((n, tok_rows), 0) == routed, 1.0, 0.0)
    earlier = one_hot(iota((tok_rows, tok_rows), 0) < iota((tok_rows, tok_rows), 1))
    before = dot(chosen.astype(bf16), earlier)
    load_of = jnp.sum(chosen, axis=1, keepdims=True)
    over = jnp.where(order < near, jnp.maximum(load_of - BLOCK, 0.0), 0.0)
    lower = one_hot(iota((n, n), 1) < iota((n, n), 0))
    start = dot(lower, over.astype(bf16))
    slot = jnp.sum(chosen * before, axis=0, keepdims=True).astype(i32)
    rank = jnp.sum(chosen * order[:, 0:1], axis=0, keepdims=True).astype(i32)
    first = jnp.sum(chosen * start[:, 0:1], axis=0, keepdims=True).astype(i32)
    far = rank < near
    direct = slot < BLOCK
    spot_s = first + slot - BLOCK
    spilled = far & (slot >= BLOCK)
    base_key = jnp.where(far & direct, rank * BLOCK + slot, none)
    far_key = jnp.where(spilled, near * BLOCK + spot_s, base_key)
    close_key = jnp.where(direct, (rank - near) * BLOCK + slot, (rank - near) * BLOCK + near * BLOCK + slot - BLOCK)
    close_key = jnp.where(far, none, close_key)
    pack_b = jnp.where(direct, rank * TILE + slot, none)
    pack_x = jnp.where(direct | far, none, (rank - near) * TILE + slot - BLOCK)
    pack_s = jnp.where(spilled, spot_s // BLOCK * TILE + spot_s % BLOCK, none)
    home = rank * TILE + extra + slot - BLOCK + 1
    lines = jnp.concatenate([pack_b, pack_x, pack_s, home, pack_b, pack_b, pack_b, pack_b], axis=0)
    cols = jnp.transpose(lines.astype(f32)).astype(i32)
    col_b, col_x, col_s, col_h = (cols[:, i:i + 1] for i in range(4))
    lane = iota((tok_rows, 128), 1)
    codes = jnp.where(col_s == lane, col_h, 0) + jnp.where(col_s + BLOCK == lane, col_h + BLOCK, 0)
    codes = jnp.sum(codes.astype(f32), axis=0, keepdims=True)
    excess = jnp.sum(over[:, 0:1], axis=0, keepdims=True) > spill * BLOCK
    excess = jnp.where(excess, 1.0, 0.0)
    note[...] = jnp.where(iota((1, 128), 1) == 127, excess, codes)

    def split(at, chunk):
        return pl.ds(pl.multiple_of(at + chunk * wide, wide), wide)

    def weave(left, right, count):
        left = left.reshape(count, BLOCK, wide)
        right = right.reshape(count, BLOCK, wide)
        return jnp.concatenate([left, right], axis=1).astype(bf16)

    tok_load.wait()
    far_hot = one_hot(far_key == iota((near * BLOCK + 2 * TILE, tok_rows), 0))

    @pl.loop(0, mid // wide)
    def _(c):
        left = dot(far_hot, tok[:, split(0, c)])
        right = dot(far_hot, tok[:, split(mid, c)])
        body = near * BLOCK
        send_b[pl.ds(0, near), :, split(0, c)] = weave(left[:body], right[:body], near)
        body, stop = near * BLOCK, near * BLOCK + spill * BLOCK
        send_s[:, :, split(0, c)] = weave(left[body:stop], right[body:stop], spill)

    pl.semaphore_wait(barrier, n - 1)
    tell(near - 1).start()
    out_s.start()

    @pl.loop(0, near)
    def _(k):
        out_b(k).start()

    close_hot = one_hot(close_key == iota((2 * near * BLOCK, tok_rows), 0))

    @pl.loop(0, mid // wide)
    def _(c):
        left = dot(close_hot, tok[:, split(0, c)])
        right = dot(close_hot, tok[:, split(mid, c)])
        body = near * BLOCK
        send_b[pl.ds(near, near), :, split(0, c)] = weave(left[:body], right[:body], near)
        send_x[:, :, split(0, c)] = weave(left[body:], right[body:], near)

    @pl.loop(near, n - 1)
    def _(k):
        out_b(k).start()

    recv_b[n - 1] = send_b[n - 1]

    tell(near - 1).wait_recv()
    out_s.wait_recv()
    code = notes[near - 1]
    depth_s = spill * TILE
    placed = code[:, :depth_s].astype(i32) - 1
    place_hot = one_hot(placed == iota((near * TILE, depth_s), 0))

    @pl.loop(0, mid // wide)
    def _(c):
        moved = dot(place_hot, recv_s[:, :, split(0, c)].reshape(depth_s, wide))
        mine = send_x[:, :, split(0, c)].reshape(near * TILE, wide).astype(f32)
        send_x[:, :, split(0, c)] = (mine + moved).astype(bf16).reshape(near, TILE, wide)

    @pl.loop(0, near - 1)
    def _(k):
        out_x(k).start()

    recv_x[near - 1] = send_x[near - 1]

    @pl.loop(0, near - 1)
    def _(k):
        tell(k).start()

    @pl.loop(near, n - 1)
    def _(k):
        tell(k).start()

    diagonal = iota((depth_s, 128), 0) == iota((depth_s, 128), 1)
    wanted = jnp.sum(jnp.where(diagonal, code, 0.0), axis=1, keepdims=True).astype(i32) - 1
    fetch_hot = one_hot(wanted == iota((depth_s, near * TILE), 1))

    for load in loads:
        load.wait()

    def ffn(arrived, result, base, count):
        rows = count * BLOCK

        @pl.loop(0, mid // wide)
        def _(c):
            piece = arrived[pl.ds(base, count), :, split(0, c)].astype(f32)
            rows_x[:rows, split(0, c)] = piece[:, :BLOCK].reshape(rows, wide).astype(bf16)
            rows_x[:rows, split(mid, c)] = piece[:, BLOCK:].reshape(rows, wide).astype(bf16)

        step = 256

        @pl.loop(0, ff // step)
        def _(f):
            at = pl.ds(pl.multiple_of(f * step, step), step)
            g_out = dot(rows_x[:rows, :], gate[:, at])
            u_out = dot(rows_x[:rows, :], up[:, at])
            hidden[:rows, at] = (jax.nn.silu(g_out) * u_out).astype(bf16)

        @pl.loop(0, mid // wide)
        def _(c):
            left = dot(hidden[:rows, :], down[:, split(0, c)])
            right = dot(hidden[:rows, :], down[:, split(mid, c)])
            result[pl.ds(base, count), :, split(0, c)] = weave(left, right, count)

    def each(first, last, act):
        @pl.loop(first, last)
        def _(k):
            act(k)

    def unpack(col, returned, base, count, start, ship):
        depth_k = count * TILE
        at = iota((tok_rows, depth_k), 1) + base * TILE
        left_hot = one_hot(col == at)
        right_hot = one_hot(col + BLOCK == at)

        @pl.loop(0, mid // wide)
        def _(c):
            piece = returned[pl.ds(base, count), :, split(0, c)].reshape(depth_k, wide)
            for hot, half in ((left_hot, 0), (right_hot, mid)):
                got = dot(hot, piece).astype(bf16)
                total[:, split(half, c)] = got if start else total[:, split(half, c)] + got
                if ship:
                    written(half, c).start()

    def written(half, c):
        at = split(half, c)
        sem = out_sem.at[half // mid, c]
        return pltpu.make_async_copy(total.at[:, at], out_hbm.at[:, at], sem)

    each(near, n - 1, lambda k: out_b(k).wait_recv())
    ffn(recv_b, res_b, near, near)
    each(near, n - 1, lambda k: back_b(k).start())
    ret_b[n - 1] = res_b[n - 1]
    each(0, near // 2, lambda k: out_b(k).wait_recv())
    ffn(recv_b, res_b, 0, near // 2)
    each(0, near // 2, lambda k: back_b(k).start())
    each(0, near - 1, lambda k: out_x(k).wait_recv())
    ffn(recv_x, res_x, 0, near)
    each(0, near - 1, lambda k: back_x(k).start())
    ret_x[near - 1] = res_x[near - 1]
    each(near // 2, near, lambda k: out_b(k).wait_recv())
    ffn(recv_b, res_b, near // 2, near // 2)
    each(near // 2, near, lambda k: back_b(k).start())

    each(0, near - 1, lambda k: back_x(k).wait_recv())

    @pl.loop(0, mid // wide)
    def _(c):
        piece = ret_x[:, :, split(0, c)].reshape(near * TILE, wide)
        res_s[:, :, split(0, c)] = dot(fetch_hot, piece).astype(bf16).reshape(spill, TILE, wide)

    back_s.start()
    unpack(col_x, ret_x, 0, near, True, False)
    each(near, n - 1, lambda k: back_b(k).wait_recv())
    unpack(col_b, ret_b, near, near, False, False)
    each(0, near - 1, lambda k: tell(k).wait_recv())
    each(near, n - 1, lambda k: tell(k).wait_recv())
    notes[n - 1] = note[...]
    worst = jnp.max(notes[...], axis=0)
    flag_ref[...] = jnp.broadcast_to(worst, flag_ref.shape)
    each(0, near // 2, lambda k: back_b(k).wait_recv())
    unpack(col_b, ret_b, 0, near // 2, False, False)
    each(near // 2, near, lambda k: back_b(k).wait_recv())
    unpack(col_b, ret_b, near // 2, near // 2, False, False)
    back_s.wait_recv()
    unpack(col_s, ret_s, 0, spill, False, True)

    each(0, n - 1, lambda k: out_b(k).wait_send())
    each(0, n - 1, lambda k: back_b(k).wait_send())
    each(0, n - 1, lambda k: tell(k).wait_send())
    each(0, near - 1, lambda k: out_x(k).wait_send())
    each(0, near - 1, lambda k: back_x(k).wait_send())
    out_s.wait_send()
    back_s.wait_send()

    @pl.loop(0, mid // wide)
    def _(c):
        written(0, c).wait()
        written(mid, c).wait()


def spilling(tokens, routed, w_gate, w_up, w_down, pairs, eps):
    n = pairs * eps
    near = n // 2
    tok_rows, depth = tokens.shape
    ff = w_gate.shape[2]
    spill = 3
    bf16, f32 = jnp.bfloat16, jnp.float32
    vmem = pl.BlockSpec(memory_space=pltpu.VMEM)
    hbm = pl.BlockSpec(memory_space=pl.ANY)
    dma = pltpu.SemaphoreType.DMA

    def blocks(count):
        return pltpu.VMEM((count, TILE, depth // 2), bf16)

    return pl.pallas_call(
        functools.partial(near_ffn, pairs, eps, spill),
        out_shape=[
            jax.ShapeDtypeStruct((tok_rows, depth), bf16),
            jax.ShapeDtypeStruct((8, 128), f32),
        ],
        in_specs=[vmem, hbm, hbm, hbm, hbm],
        out_specs=[hbm, vmem],
        scratch_shapes=[
            pltpu.VMEM((tok_rows, depth), bf16),
            *[blocks(n)] * 4,
            *[blocks(near)] * 4,
            *[blocks(spill)] * 4,
            pltpu.VMEM((1, 128), f32),
            pltpu.VMEM((n, 1, 128), f32),
            pltpu.VMEM((depth, ff), bf16),
            pltpu.VMEM((depth, ff), bf16),
            pltpu.VMEM((ff, depth), bf16),
            pltpu.VMEM((near * BLOCK, depth), bf16),
            pltpu.VMEM((near * BLOCK, ff), bf16),
            pltpu.VMEM((tok_rows, depth), bf16),
            dma((1,)), dma((3,)), dma((2, depth // 2 // 512)),
            dma((2, n)), dma((2, n)), dma((2, near)), dma((2, near)),
            dma((2,)), dma((2,)), dma((n,)), dma((n,)),
        ],
        compiler_params=pltpu.CompilerParams(
            collective_id=1, has_side_effects=True, vmem_limit_bytes=56 * 1024 * 1024
        ),
        name="near_ffn",
    )(routed.reshape(1, tok_rows), tokens, w_gate, w_up, w_down)


def dispatch(tokens, routed, w_gate, w_up, w_down, pairs, eps):
    experts = pairs * eps
    tok_rows, depth = tokens.shape
    cap = tok_rows // experts + tok_rows // (2 * experts)
    onehot = (routed[:, None] == jnp.arange(experts, dtype=jnp.int32)[None, :]).astype(jnp.float32)
    order = jnp.arange(tok_rows)
    earlier = (order[:, None] > order[None, :]).astype(jnp.bfloat16)
    before = dot(earlier, onehot.astype(jnp.bfloat16))
    slot = jnp.sum(before * onehot, axis=1).astype(jnp.int32)
    spare = TILE - cap
    packs = 0 < spare <= cap and cap % spare == 0 and (depth * spare) % (TILE * 256) == 0
    if packs and experts % GROUP == 0 and w_gate.shape[2] % 256 == 0:
        return fused(tokens, routed, slot, w_gate, w_up, w_down, pairs, eps, cap)
    return plain(tokens, routed, slot, w_gate, w_up, w_down, experts, cap)


def shards(tokens, expert_of, w_gate, w_up, w_down):
    pairs = lax.axis_size("pair")
    eps = lax.axis_size("ep")
    experts = pairs * eps
    tok_rows, depth = tokens.shape
    routed = expert_of[:, 0]
    whole = (tokens, routed, w_gate, w_up, w_down)
    even = tok_rows == BLOCK * experts and eps % 2 == 0 and experts % (2 * GROUP) == 0
    if not (even and depth % 1024 == 0 and w_gate.shape[2] % 256 == 0):
        return dispatch(*whole, pairs, eps)
    result, flag = spilling(*whole, pairs, eps)
    return lax.cond(
        flag[0, 127] > 0,
        lambda: dispatch(*whole, pairs, eps),
        lambda: result,
    )


def solution(mesh):
    spec2 = P(("pair", "ep"), None)
    spec3 = P(("pair", "ep"), None, None)
    return jax.shard_map(
        shards,
        mesh=mesh,
        in_specs=(spec2, spec2, spec3, spec3, spec3),
        out_specs=spec2,
        check_vma=False,
    )
```

```python
import functools

import jax
import jax.numpy as jnp
from jax import lax
from jax.experimental import pallas as pl
from jax.experimental.pallas import tpu as pltpu
from jax.sharding import PartitionSpec as P

MESH = pl.DeviceIdType.MESH
TILE = 16
GROUP = 8


def dot(a, b):
    return jnp.dot(a, b, preferred_element_type=jnp.float32)


def exchange_ffn(
    pairs, eps, cap, row_keys, col_keys, tok_hbm, gate_hbm, up_hbm, down_hbm, head_ref, ends_ref,
    tok, outgoing, recv, result, returned, gate, up, down, hidden, rest,
    tok_sem, w_sem, local_sem, send1, recv1, send2, recv2,
):
    n = pairs * eps
    pair, ep = lax.axis_index("pair"), lax.axis_index("ep")
    tok_rows = tok.shape[0]
    width = recv.shape[2]
    tail = rest.shape[1]
    parts = cap // (TILE - cap)
    spare = TILE - cap
    rows = GROUP * TILE
    bf16 = jnp.bfloat16

    def shift(k):
        i = k // pairs
        de = (eps // 2 + ((i + 1) // 2) * (2 * ((i + 1) % 2) - 1) + eps) % eps
        return (k + 1) % pairs, de

    def target(k):
        dp, de = shift(k)
        return lax.rem(pair + dp, pairs), lax.rem(ep + de, eps)

    def origin(k):
        dp, de = shift(k)
        return lax.rem(pair + pairs - dp, pairs), lax.rem(ep + eps - de, eps)

    tok_load = pltpu.make_async_copy(tok_hbm, tok, tok_sem.at[0])
    tok_load.start()

    barrier = pltpu.get_barrier_semaphore()

    @pl.loop(0, n - 1)
    def _(k):
        p, e = target(k)
        pl.semaphore_signal(barrier, inc=1, device_id=(p, e), device_id_type=MESH)

    loads = [
        pltpu.make_async_copy(src.at[0], dst, w_sem.at[i])
        for i, (src, dst) in enumerate(((gate_hbm, gate), (up_hbm, up), (down_hbm, down)))
    ]
    for load in loads:
        load.start()

    def outbound(k):
        p, e = target(k)
        return pltpu.make_async_remote_copy(
            src_ref=outgoing.at[k],
            dst_ref=recv.at[k],
            send_sem=send1.at[k],
            recv_sem=recv1.at[k],
            device_id=(p, e),
            device_id_type=MESH,
        )

    def inbound(k):
        p, e = origin(k)
        return pltpu.make_async_remote_copy(
            src_ref=result.at[k],
            dst_ref=returned.at[k],
            send_sem=send2.at[k],
            recv_sem=recv2.at[k],
            device_id=(p, e),
            device_id_type=MESH,
        )

    def row_ids(first, shape, axis):
        at = lax.broadcasted_iota(jnp.int32, shape, axis)
        base = jnp.zeros(shape, jnp.int32)
        for i in range(GROUP):
            p, e = target(first + i)
            base = jnp.where(at // TILE == i, (p * eps + e) * TILE, base)
        return base + at % TILE

    def one_hot(mask):
        return mask.astype(jnp.float32).astype(bf16)

    def pack(first):
        ids = row_ids(first, (rows, tok_rows), 0)
        main = one_hot(row_keys[0:1, :] == ids)
        for j in range(parts):
            cols = pl.ds(j * tail, tail)
            ends = one_hot(row_keys[j + 1:j + 2, :] == ids)
            piece = dot(main, tok[:, cols]) + dot(ends, tok[:, width:])
            outgoing[pl.ds(first, GROUP), :, cols] = piece.astype(bf16).reshape(GROUP, TILE, tail)

    def unpack(first, start):
        ids = row_ids(first, (tok_rows, rows), 1)
        main = one_hot(col_keys[:, 0:1] == ids)
        ends = jnp.zeros((tok_rows, tail), jnp.float32)
        for j in range(parts):
            cols = pl.ds(j * tail, tail)
            piece = returned[pl.ds(first, GROUP), :, cols].reshape(rows, tail)
            head = dot(main, piece).astype(bf16)
            head_ref[:, cols] = head if start else head_ref[:, cols] + head
            ends = ends + dot(one_hot(col_keys[:, j + 1:j + 2] == ids), piece)
        ends = ends.astype(bf16)
        ends_ref[...] = ends if start else ends_ref[...] + ends

    def send(first):
        @pl.loop(0, GROUP)
        def _(i):
            @pl.when(first + i < n - 1)
            def _():
                outbound(first + i).start()

    tok_load.wait()
    pack(0)
    pl.semaphore_wait(barrier, n - 1)
    send(0)

    @pl.loop(1, n // GROUP)
    def _(g):
        pack(g * GROUP)
        send(g * GROUP)

    own = pltpu.make_async_copy(outgoing.at[n - 1], recv.at[n - 1], local_sem.at[0])
    own.start()
    for load in loads:
        load.wait()
    own.wait()

    r = lax.broadcasted_iota(jnp.int32, (rows, rows), 0)
    c = lax.broadcasted_iota(jnp.int32, (rows, rows), 1)
    same = (r // TILE) == (c // TILE)
    r, c = r % TILE, c % TILE

    def spreader(j):
        return one_hot(same & (r // spare == j) & (c == cap + r % spare))

    def folder(j):
        return one_hot(same & (r >= cap) & (c == spare * j + r - cap))

    body_row = (lax.broadcasted_iota(jnp.int32, (rows, 1), 0) % TILE) < cap
    step = 256

    @pl.loop(0, n // GROUP)
    def _(g):
        first = g * GROUP

        @pl.loop(0, GROUP)
        def _(i):
            @pl.when(first + i < n - 1)
            def _():
                outbound(first + i).wait_recv()

        block = recv.at[pl.ds(first, GROUP)]
        total = jnp.zeros((rows, tail), jnp.float32)
        for j in range(parts):
            piece = block[:, :, j * tail:(j + 1) * tail].reshape(rows, tail)
            total = total + dot(spreader(j), piece)
        rest[...] = total.astype(bf16)

        @pl.loop(0, hidden.shape[1] // step)
        def _(f):
            cols = pl.ds(pl.multiple_of(f * step, step), step)
            main = block[...].reshape(rows, width)
            g_out = dot(main, gate[:width, cols]) + dot(rest[...], gate[width:, cols])
            u_out = dot(main, up[:width, cols]) + dot(rest[...], up[width:, cols])
            hidden[:, cols] = (jax.nn.silu(g_out) * u_out).astype(bf16)

        rest[...] = dot(hidden[...], down[:, width:]).astype(bf16)
        for j in range(parts):
            cols = pl.ds(j * tail, tail)
            body = dot(hidden[...], down[:, cols])
            extra = dot(folder(j), rest[...])
            packed = jnp.where(body_row, body, extra).astype(bf16)
            result[pl.ds(first, GROUP), :, cols] = packed.reshape(GROUP, TILE, tail)

        @pl.loop(0, GROUP)
        def _(i):
            @pl.when(first + i < n - 1)
            def _():
                inbound(first + i).start()

    mine = pltpu.make_async_copy(result.at[n - 1], returned.at[n - 1], local_sem.at[1])
    mine.start()
    mine.wait()

    def collect(first):
        @pl.loop(0, GROUP)
        def _(i):
            @pl.when(first + i < n - 1)
            def _():
                inbound(first + i).wait_recv()

    collect(0)
    unpack(0, True)

    @pl.loop(1, n // GROUP)
    def _(g):
        collect(g * GROUP)
        unpack(g * GROUP, False)

    @pl.loop(0, n - 1)
    def _(k):
        outbound(k).wait_send()
        inbound(k).wait_send()


def fused(tokens, routed, slot, w_gate, w_up, w_down, pairs, eps, cap):
    n = pairs * eps
    tok_rows, depth = tokens.shape
    ff = w_gate.shape[2]
    spare = TILE - cap
    parts = cap // spare
    tail = depth * spare // TILE
    width = depth - tail

    rest_key = jnp.where(
        slot[None, :] // spare == jnp.arange(parts)[:, None],
        (routed * TILE + cap + slot % spare)[None, :],
        -1,
    )
    keys = jnp.concatenate([(routed * TILE + slot)[None, :], rest_key], axis=0)

    vmem = pl.BlockSpec(memory_space=pltpu.VMEM)
    hbm = pl.BlockSpec(memory_space=pl.ANY)
    bf16 = jnp.bfloat16
    parcels = pltpu.VMEM((n, TILE, width), bf16)
    head, ends = pl.pallas_call(
        functools.partial(exchange_ffn, pairs, eps, cap),
        out_shape=[
            jax.ShapeDtypeStruct((tok_rows, width), bf16),
            jax.ShapeDtypeStruct((tok_rows, tail), bf16),
        ],
        in_specs=[vmem, vmem, hbm, hbm, hbm, hbm],
        out_specs=[vmem, vmem],
        scratch_shapes=[
            pltpu.VMEM((tok_rows, depth), bf16),
            parcels,
            parcels,
            parcels,
            parcels,
            pltpu.VMEM((depth, ff), bf16),
            pltpu.VMEM((depth, ff), bf16),
            pltpu.VMEM((ff, depth), bf16),
            pltpu.VMEM((GROUP * TILE, ff), bf16),
            pltpu.VMEM((GROUP * TILE, tail), bf16),
            pltpu.SemaphoreType.DMA((1,)),
            pltpu.SemaphoreType.DMA((3,)),
            pltpu.SemaphoreType.DMA((2,)),
            pltpu.SemaphoreType.DMA((n,)),
            pltpu.SemaphoreType.DMA((n,)),
            pltpu.SemaphoreType.DMA((n,)),
            pltpu.SemaphoreType.DMA((n,)),
        ],
        compiler_params=pltpu.CompilerParams(
            collective_id=0, has_side_effects=True, vmem_limit_bytes=56 * 1024 * 1024
        ),
        name="exchange_ffn",
    )(keys, keys.T, tokens, w_gate, w_up, w_down)
    return jnp.concatenate([head, ends], axis=1)


def plain(tokens, routed, slot, w_gate, w_up, w_down, experts, capacity):
    position = routed * capacity + slot
    outgoing = (
        jnp.zeros((experts * capacity, tokens.shape[1]), jnp.bfloat16).at[position].set(tokens)
    )
    parcel = lax.all_to_all(
        outgoing.reshape(experts, capacity, outgoing.shape[1]),
        ("pair", "ep"), split_axis=0, concat_axis=0, tiled=True,
    )
    flat_rows = parcel.reshape(experts * capacity, parcel.shape[2])
    gate_proj = dot(flat_rows, w_gate[0])
    up_proj = dot(flat_rows, w_up[0])
    hidden = (jax.nn.silu(gate_proj) * up_proj).astype(jnp.bfloat16)
    result = dot(hidden, w_down[0]).astype(jnp.bfloat16)
    returned = lax.all_to_all(
        result.reshape(experts, capacity, result.shape[1]),
        ("pair", "ep"), split_axis=0, concat_axis=0, tiled=True,
    )
    return jnp.take(returned.reshape(experts * capacity, -1), position, axis=0)


BLOCK = 8


def near_ffn(
    pairs, eps, spill, keys_hbm, tok_hbm, gate_hbm, up_hbm, down_hbm, total, flag_ref,
    tok, send_b, recv_b, res_b, ret_b, send_x, recv_x, res_x, ret_x, send_s, recv_s, res_s, ret_s,
    keys_ref, note, notes, gate, up, down, rows_x, hidden,
    load_sem, w_sem, ssem, rsem,
):
    n = pairs * eps
    near = n // 2
    line = eps // 2
    pair, ep = lax.axis_index("pair"), lax.axis_index("ep")
    side, spot = ep // line, ep % line
    tok_rows, depth = tok.shape
    mid = depth // 2
    ff = hidden.shape[1]
    extra = BLOCK // 2
    bf16, f32, i32 = jnp.bfloat16, jnp.float32, jnp.int32
    none = -4 * n * TILE
    wide = 512

    def peer(k, sign):
        j = k % near + 1
        p = lax.rem(pair + pairs + sign * (j // line % pairs), pairs)
        s = lax.rem(spot + line + sign * (j % line), line)
        return p, lax.rem(side + 1 - k // near, 2) * line + s

    key_load = pltpu.make_async_copy(keys_hbm, keys_ref, load_sem.at[0])
    key_load.start()
    tok_load = pltpu.make_async_copy(tok_hbm, tok, load_sem.at[1])
    tok_load.start()
    barrier = pltpu.get_barrier_semaphore()

    @pl.loop(0, n - 1)
    def _(k):
        pl.semaphore_signal(barrier, inc=1, device_id=peer(k, 1), device_id_type=MESH)

    loads = [
        pltpu.make_async_copy(src.at[0], dst, w_sem.at[i])
        for i, (src, dst) in enumerate(((gate_hbm, gate), (up_hbm, up), (down_hbm, down)))
    ]

    half = near // 2
    groups = {
        "far_a": (send_b, recv_b, 0, half),
        "far_b": (send_b, recv_b, half, near),
        "close": (send_b, recv_b, near, n - 1),
        "extra": (send_x, recv_x, 0, near - 1),
        "spill": (send_s, recv_s, 0, spill),
        "back_far_a": (res_b, ret_b, 0, half),
        "back_far_b": (res_b, ret_b, half, near),
        "back_close": (res_b, ret_b, near, n - 1),
        "back_extra": (res_x, ret_x, 0, near - 1),
        "back_spill": (res_s, ret_s, 0, spill),
    }
    ports = {name: i for i, name in enumerate(groups)}

    def remote(name, src, dst, to, part=0):
        at = ports[name] + part
        return pltpu.make_async_remote_copy(
            src_ref=src, dst_ref=dst, send_sem=ssem.at[at], recv_sem=rsem.at[at],
            device_id=to, device_id_type=MESH,
        )

    mirror = (pair, lax.rem(side + 1, 2) * line + spot)

    def go(name):
        src, dst, low, high = groups[name]
        if src.shape[0] == spill:
            remote(name, src, dst, mirror).start()
            return
        sign = -1 if name[:4] == "back" else 1
        skip = near if src.shape[0] == near else 0

        @pl.loop(low, high)
        def _(k):
            remote(name, src.at[k], dst.at[k], peer(k + skip, sign)).start()

    def group(name):
        src, dst, low, high = groups[name]
        part = pl.ds(low, high - low)
        return remote(name, src.at[part], dst.at[part], mirror)

    last = len(groups)

    def tell(k, part):
        return pltpu.make_async_remote_copy(
            src_ref=note, dst_ref=notes.at[k], send_sem=ssem.at[last + part],
            recv_sem=rsem.at[last + part], device_id=peer(k, 1), device_id_type=MESH,
        )

    def told(low, high, part):
        some = notes.at[pl.ds(low, high - low)]
        return pltpu.make_async_remote_copy(
            src_ref=some, dst_ref=some, send_sem=ssem.at[last + part],
            recv_sem=rsem.at[last + part], device_id=mirror, device_id_type=MESH,
        )

    def iota(shape, axis):
        return lax.broadcasted_iota(i32, shape, axis)

    def one_hot(mask):
        return jnp.where(mask, 1.0, 0.0).astype(bf16)

    expert = iota((n, 128), 0)
    order = jnp.zeros((n, 128), i32)
    for k in range(n):
        p, e = peer(k, 1) if k < n - 1 else (pair, ep)
        order = jnp.where(expert == p * eps + e, k, order)
    order = order.astype(f32)
    key_load.wait()
    routed = keys_ref[...]
    which = iota((n, tok_rows), 0)
    chosen = jnp.where(which == routed, 1.0, 0.0)
    earlier = one_hot(iota((tok_rows, tok_rows), 0) < iota((tok_rows, tok_rows), 1))
    before = dot(chosen.astype(bf16), earlier)
    load_of = jnp.sum(chosen, axis=1, keepdims=True)
    over = jnp.where(order < near, jnp.maximum(load_of - BLOCK, 0.0), 0.0)
    ahead = jnp.where(which < routed, over[:, 0:1], 0.0)
    first = jnp.sum(ahead, axis=0, keepdims=True).astype(i32)
    rank = jnp.sum(chosen * order[:, 0:1], axis=0, keepdims=True).astype(i32)
    slot = jnp.sum(chosen * before, axis=0, keepdims=True).astype(i32)
    far = rank < near
    direct = slot < BLOCK
    spot_s = first + slot - BLOCK
    spilled = far & (slot >= BLOCK)
    spill_key = jnp.where(spilled, spot_s, none)

    def split(at, chunk):
        return pl.ds(pl.multiple_of(at + chunk * wide, wide), wide)

    def weave(left, right, count):
        left = left.reshape(count, BLOCK, wide)
        right = right.reshape(count, BLOCK, wide)
        return jnp.concatenate([left, right], axis=1).astype(bf16)

    tok_load.wait()
    for load in loads:
        load.start()

    spill_hot = one_hot(spill_key == iota((spill * BLOCK, tok_rows), 0))

    @pl.loop(0, mid // wide)
    def _(c):
        left = dot(spill_hot, tok[:, split(0, c)])
        right = dot(spill_hot, tok[:, split(mid, c)])
        send_s[:, :, split(0, c)] = weave(left, right, spill)

    pl.semaphore_wait(barrier, n - 1)
    go("spill")

    far_key = jnp.where(far & direct, rank * BLOCK + slot, none)
    beyond = jnp.where(direct, slot, near * BLOCK + slot - BLOCK)
    close_key = jnp.where(far, none, (rank - near) * BLOCK + beyond)
    pack_b = jnp.where(direct, rank * TILE + slot, none)
    pack_x = jnp.where(direct | far, none, (rank - near) * TILE + slot - BLOCK)
    pack_s = jnp.where(spilled, spot_s // BLOCK * TILE + spot_s % BLOCK, none)
    home = rank * TILE + extra + slot - BLOCK + 1
    lines = jnp.concatenate([pack_b, pack_x, pack_s, home, pack_b, pack_b, pack_b, pack_b], axis=0)
    cols = jnp.transpose(lines.astype(f32)).astype(i32)
    col_b, col_x, col_s, col_h = (cols[:, i:i + 1] for i in range(4))
    lane = iota((tok_rows, 128), 1)
    codes = jnp.where(col_s == lane, col_h, 0) + jnp.where(col_s + BLOCK == lane, col_h + BLOCK, 0)
    codes = jnp.sum(codes.astype(f32), axis=0, keepdims=True)
    excess = jnp.sum(over[:, 0:1], axis=0, keepdims=True) > spill * BLOCK
    excess = jnp.where(excess, 1.0, 0.0)
    note[...] = jnp.where(iota((1, 128), 1) == 127, excess, codes)

    tell(near - 1, 0).start()
    far_hot = one_hot(far_key == iota((near * BLOCK, tok_rows), 0))

    @pl.loop(0, mid // wide)
    def _(c):
        left = dot(far_hot, tok[:, split(0, c)])
        right = dot(far_hot, tok[:, split(mid, c)])
        send_b[pl.ds(0, near), :, split(0, c)] = weave(left, right, near)

    go("far_a")
    go("far_b")

    close_hot = one_hot(close_key == iota((2 * near * BLOCK, tok_rows), 0))

    @pl.loop(0, mid // wide)
    def _(c):
        left = dot(close_hot, tok[:, split(0, c)])
        right = dot(close_hot, tok[:, split(mid, c)])
        body = near * BLOCK
        send_b[pl.ds(near, near), :, split(0, c)] = weave(left[:body], right[:body], near)
        send_x[:, :, split(0, c)] = weave(left[body:], right[body:], near)

    go("close")

    recv_b[n - 1] = send_b[n - 1]

    tell(near - 1, 0).wait_recv()
    group("spill").wait_recv()
    code = notes[near - 1]
    depth_s = spill * TILE
    placed = code[:, :depth_s].astype(i32) - 1
    place_hot = one_hot(placed == iota((near * TILE, depth_s), 0))

    @pl.loop(0, mid // wide)
    def _(c):
        moved = dot(place_hot, recv_s[:, :, split(0, c)].reshape(depth_s, wide))
        mine = send_x[:, :, split(0, c)].reshape(near * TILE, wide).astype(f32)
        send_x[:, :, split(0, c)] = (mine + moved).astype(bf16).reshape(near, TILE, wide)

    go("extra")
    recv_x[near - 1] = send_x[near - 1]

    @pl.loop(0, near - 1)
    def _(k):
        tell(k, 1).start()

    @pl.loop(near, n - 1)
    def _(k):
        tell(k, 2).start()

    diagonal = iota((depth_s, 128), 0) == iota((depth_s, 128), 1)
    wanted = jnp.sum(jnp.where(diagonal, code, 0.0), axis=1, keepdims=True).astype(i32) - 1
    fetch_hot = one_hot(wanted == iota((depth_s, near * TILE), 1))

    for load in loads:
        load.wait()

    def ffn(arrived, result, base, count):
        rows = count * BLOCK

        @pl.loop(0, mid // wide)
        def _(c):
            piece = arrived[pl.ds(base, count), :, split(0, c)].astype(f32)
            rows_x[:rows, split(0, c)] = piece[:, :BLOCK].reshape(rows, wide).astype(bf16)
            rows_x[:rows, split(mid, c)] = piece[:, BLOCK:].reshape(rows, wide).astype(bf16)

        step = 256

        @pl.loop(0, ff // step)
        def _(f):
            at = pl.ds(pl.multiple_of(f * step, step), step)
            g_out = dot(rows_x[:rows, :], gate[:, at])
            u_out = dot(rows_x[:rows, :], up[:, at])
            hidden[:rows, at] = (jax.nn.silu(g_out) * u_out).astype(bf16)

        @pl.loop(0, mid // wide)
        def _(c):
            left = dot(hidden[:rows, :], down[:, split(0, c)])
            right = dot(hidden[:rows, :], down[:, split(mid, c)])
            result[pl.ds(base, count), :, split(0, c)] = weave(left, right, count)

    def unpack(col, returned, base, count, start):
        depth_k = count * TILE
        at = iota((tok_rows, depth_k), 1) + base * TILE
        left_hot = one_hot(col == at)
        right_hot = one_hot(col + BLOCK == at)

        @pl.loop(0, mid // wide)
        def _(c):
            piece = returned[pl.ds(base, count), :, split(0, c)].reshape(depth_k, wide)
            for hot, half in ((left_hot, 0), (right_hot, mid)):
                got = dot(hot, piece).astype(bf16)
                total[:, split(half, c)] = got if start else total[:, split(half, c)] + got

    group("close").wait_recv()
    ffn(recv_b, res_b, near, near)
    go("back_close")
    ret_b[n - 1] = res_b[n - 1]
    group("far_a").wait_recv()
    ffn(recv_b, res_b, 0, half)
    go("back_far_a")
    group("extra").wait_recv()
    ffn(recv_x, res_x, 0, near)
    go("back_extra")
    ret_x[near - 1] = res_x[near - 1]
    group("far_b").wait_recv()
    ffn(recv_b, res_b, half, half)
    go("back_far_b")

    for name in ("spill", "far_a", "far_b", "close", "extra"):
        group(name).wait_send()
    tell(near - 1, 0).wait_send()
    told(0, near - 1, 1).wait_send()
    told(near, n - 1, 2).wait_send()
    group("back_extra").wait_recv()

    @pl.loop(0, mid // wide)
    def _(c):
        piece = ret_x[:, :, split(0, c)].reshape(near * TILE, wide)
        res_s[:, :, split(0, c)] = dot(fetch_hot, piece).astype(bf16).reshape(spill, TILE, wide)

    go("back_spill")
    unpack(col_x, ret_x, 0, near, True)
    group("back_close").wait_recv()
    unpack(col_b, ret_b, near, near, False)
    told(0, near - 1, 1).wait_recv()
    told(near, n - 1, 2).wait_recv()
    notes[n - 1] = note[...]
    worst = jnp.where(iota((1, 128), 1) == 127, jnp.max(notes[...], axis=0), 0.0)
    flag_ref[0, 0] = jnp.max(worst)
    group("back_far_a").wait_recv()
    unpack(col_b, ret_b, 0, half, False)
    group("back_far_b").wait_recv()
    unpack(col_b, ret_b, half, half, False)
    group("back_spill").wait_recv()
    unpack(col_s, ret_s, 0, spill, False)
    for name in ("back_close", "back_far_a", "back_extra", "back_far_b", "back_spill"):
        group(name).wait_send()


def spilling(tokens, routed, w_gate, w_up, w_down, pairs, eps):
    n = pairs * eps
    near = n // 2
    tok_rows, depth = tokens.shape
    ff = w_gate.shape[2]
    spill = 3
    bf16, f32 = jnp.bfloat16, jnp.float32
    vmem = pl.BlockSpec(memory_space=pltpu.VMEM)
    hbm = pl.BlockSpec(memory_space=pl.ANY)
    dma = pltpu.SemaphoreType.DMA

    def blocks(count):
        return pltpu.VMEM((count, TILE, depth // 2), bf16)

    return pl.pallas_call(
        functools.partial(near_ffn, pairs, eps, spill),
        out_shape=[
            jax.ShapeDtypeStruct((tok_rows, depth), bf16),
            jax.ShapeDtypeStruct((1, 1), f32),
        ],
        in_specs=[hbm, hbm, hbm, hbm, hbm],
        out_specs=[vmem, pl.BlockSpec(memory_space=pltpu.SMEM)],
        scratch_shapes=[
            pltpu.VMEM((tok_rows, depth), bf16),
            *[blocks(n)] * 4,
            *[blocks(near)] * 4,
            *[blocks(spill)] * 4,
            pltpu.VMEM((1, tok_rows), jnp.int32),
            pltpu.VMEM((1, 128), f32),
            pltpu.VMEM((n, 1, 128), f32),
            pltpu.VMEM((depth, ff), bf16),
            pltpu.VMEM((depth, ff), bf16),
            pltpu.VMEM((ff, depth), bf16),
            pltpu.VMEM((near * BLOCK, depth), bf16),
            pltpu.VMEM((near * BLOCK, ff), bf16),
            dma((2,)), dma((3,)), dma((13,)), dma((13,)),
        ],
        compiler_params=pltpu.CompilerParams(
            collective_id=1, has_side_effects=True, vmem_limit_bytes=56 * 1024 * 1024
        ),
        name="near_ffn",
    )(routed.reshape(1, tok_rows), tokens, w_gate, w_up, w_down)


def dispatch(tokens, routed, w_gate, w_up, w_down, pairs, eps):
    experts = pairs * eps
    tok_rows, depth = tokens.shape
    cap = tok_rows // experts + tok_rows // (2 * experts)
    onehot = (routed[:, None] == jnp.arange(experts, dtype=jnp.int32)[None, :]).astype(jnp.float32)
    order = jnp.arange(tok_rows)
    earlier = (order[:, None] > order[None, :]).astype(jnp.bfloat16)
    before = dot(earlier, onehot.astype(jnp.bfloat16))
    slot = jnp.sum(before * onehot, axis=1).astype(jnp.int32)
    spare = TILE - cap
    packs = 0 < spare <= cap and cap % spare == 0 and (depth * spare) % (TILE * 256) == 0
    if packs and experts % GROUP == 0 and w_gate.shape[2] % 256 == 0:
        return fused(tokens, routed, slot, w_gate, w_up, w_down, pairs, eps, cap)
    return plain(tokens, routed, slot, w_gate, w_up, w_down, experts, cap)


def shards(tokens, expert_of, w_gate, w_up, w_down):
    pairs = lax.axis_size("pair")
    eps = lax.axis_size("ep")
    experts = pairs * eps
    tok_rows, depth = tokens.shape
    routed = expert_of[:, 0]
    whole = (tokens, routed, w_gate, w_up, w_down)
    even = tok_rows == BLOCK * experts and eps % 2 == 0 and experts % (2 * GROUP) == 0
    if not (even and depth % 1024 == 0 and w_gate.shape[2] % 256 == 0):
        return dispatch(*whole, pairs, eps)
    result, flag = spilling(*whole, pairs, eps)
    return lax.cond(
        flag[0, 0] > 0,
        lambda: dispatch(*whole, pairs, eps),
        lambda: result,
    )


def solution(mesh):
    spec2 = P(("pair", "ep"), None)
    spec3 = P(("pair", "ep"), None, None)
    return jax.shard_map(
        shards,
        mesh=mesh,
        in_specs=(spec2, spec2, spec3, spec3, spec3),
        out_specs=spec2,
        check_vma=False,
    )
```

```python
import functools

import jax
import jax.numpy as jnp
from jax import lax
from jax.experimental import pallas as pl
from jax.experimental.pallas import tpu as pltpu
from jax.sharding import PartitionSpec as P

MESH = pl.DeviceIdType.MESH
TILE = 16
GROUP = 8


def dot(a, b):
    return jnp.dot(a, b, preferred_element_type=jnp.float32)


def exchange_ffn(
    pairs, eps, cap, row_keys, col_keys, tok_hbm, gate_hbm, up_hbm, down_hbm, head_ref, ends_ref,
    tok, outgoing, recv, result, returned, gate, up, down, hidden, rest,
    tok_sem, w_sem, local_sem, send1, recv1, send2, recv2,
):
    n = pairs * eps
    pair, ep = lax.axis_index("pair"), lax.axis_index("ep")
    tok_rows = tok.shape[0]
    width = recv.shape[2]
    tail = rest.shape[1]
    parts = cap // (TILE - cap)
    spare = TILE - cap
    rows = GROUP * TILE
    bf16 = jnp.bfloat16

    def shift(k):
        i = k // pairs
        de = (eps // 2 + ((i + 1) // 2) * (2 * ((i + 1) % 2) - 1) + eps) % eps
        return (k + 1) % pairs, de

    def target(k):
        dp, de = shift(k)
        return lax.rem(pair + dp, pairs), lax.rem(ep + de, eps)

    def origin(k):
        dp, de = shift(k)
        return lax.rem(pair + pairs - dp, pairs), lax.rem(ep + eps - de, eps)

    tok_load = pltpu.make_async_copy(tok_hbm, tok, tok_sem.at[0])
    tok_load.start()

    barrier = pltpu.get_barrier_semaphore()

    @pl.loop(0, n - 1)
    def _(k):
        p, e = target(k)
        pl.semaphore_signal(barrier, inc=1, device_id=(p, e), device_id_type=MESH)

    loads = [
        pltpu.make_async_copy(src.at[0], dst, w_sem.at[i])
        for i, (src, dst) in enumerate(((gate_hbm, gate), (up_hbm, up), (down_hbm, down)))
    ]
    for load in loads:
        load.start()

    def outbound(k):
        p, e = target(k)
        return pltpu.make_async_remote_copy(
            src_ref=outgoing.at[k],
            dst_ref=recv.at[k],
            send_sem=send1.at[k],
            recv_sem=recv1.at[k],
            device_id=(p, e),
            device_id_type=MESH,
        )

    def inbound(k):
        p, e = origin(k)
        return pltpu.make_async_remote_copy(
            src_ref=result.at[k],
            dst_ref=returned.at[k],
            send_sem=send2.at[k],
            recv_sem=recv2.at[k],
            device_id=(p, e),
            device_id_type=MESH,
        )

    def row_ids(first, shape, axis):
        at = lax.broadcasted_iota(jnp.int32, shape, axis)
        base = jnp.zeros(shape, jnp.int32)
        for i in range(GROUP):
            p, e = target(first + i)
            base = jnp.where(at // TILE == i, (p * eps + e) * TILE, base)
        return base + at % TILE

    def one_hot(mask):
        return mask.astype(jnp.float32).astype(bf16)

    def pack(first):
        ids = row_ids(first, (rows, tok_rows), 0)
        main = one_hot(row_keys[0:1, :] == ids)
        for j in range(parts):
            cols = pl.ds(j * tail, tail)
            ends = one_hot(row_keys[j + 1:j + 2, :] == ids)
            piece = dot(main, tok[:, cols]) + dot(ends, tok[:, width:])
            outgoing[pl.ds(first, GROUP), :, cols] = piece.astype(bf16).reshape(GROUP, TILE, tail)

    def unpack(first, start):
        ids = row_ids(first, (tok_rows, rows), 1)
        main = one_hot(col_keys[:, 0:1] == ids)
        ends = jnp.zeros((tok_rows, tail), jnp.float32)
        for j in range(parts):
            cols = pl.ds(j * tail, tail)
            piece = returned[pl.ds(first, GROUP), :, cols].reshape(rows, tail)
            head = dot(main, piece).astype(bf16)
            head_ref[:, cols] = head if start else head_ref[:, cols] + head
            ends = ends + dot(one_hot(col_keys[:, j + 1:j + 2] == ids), piece)
        ends = ends.astype(bf16)
        ends_ref[...] = ends if start else ends_ref[...] + ends

    def send(first):
        @pl.loop(0, GROUP)
        def _(i):
            @pl.when(first + i < n - 1)
            def _():
                outbound(first + i).start()

    tok_load.wait()
    pack(0)
    pl.semaphore_wait(barrier, n - 1)
    send(0)

    @pl.loop(1, n // GROUP)
    def _(g):
        pack(g * GROUP)
        send(g * GROUP)

    own = pltpu.make_async_copy(outgoing.at[n - 1], recv.at[n - 1], local_sem.at[0])
    own.start()
    for load in loads:
        load.wait()
    own.wait()

    r = lax.broadcasted_iota(jnp.int32, (rows, rows), 0)
    c = lax.broadcasted_iota(jnp.int32, (rows, rows), 1)
    same = (r // TILE) == (c // TILE)
    r, c = r % TILE, c % TILE

    def spreader(j):
        return one_hot(same & (r // spare == j) & (c == cap + r % spare))

    def folder(j):
        return one_hot(same & (r >= cap) & (c == spare * j + r - cap))

    body_row = (lax.broadcasted_iota(jnp.int32, (rows, 1), 0) % TILE) < cap
    step = 256

    @pl.loop(0, n // GROUP)
    def _(g):
        first = g * GROUP

        @pl.loop(0, GROUP)
        def _(i):
            @pl.when(first + i < n - 1)
            def _():
                outbound(first + i).wait_recv()

        block = recv.at[pl.ds(first, GROUP)]
        total = jnp.zeros((rows, tail), jnp.float32)
        for j in range(parts):
            piece = block[:, :, j * tail:(j + 1) * tail].reshape(rows, tail)
            total = total + dot(spreader(j), piece)
        rest[...] = total.astype(bf16)

        @pl.loop(0, hidden.shape[1] // step)
        def _(f):
            cols = pl.ds(pl.multiple_of(f * step, step), step)
            main = block[...].reshape(rows, width)
            g_out = dot(main, gate[:width, cols]) + dot(rest[...], gate[width:, cols])
            u_out = dot(main, up[:width, cols]) + dot(rest[...], up[width:, cols])
            hidden[:, cols] = (jax.nn.silu(g_out) * u_out).astype(bf16)

        rest[...] = dot(hidden[...], down[:, width:]).astype(bf16)
        for j in range(parts):
            cols = pl.ds(j * tail, tail)
            body = dot(hidden[...], down[:, cols])
            extra = dot(folder(j), rest[...])
            packed = jnp.where(body_row, body, extra).astype(bf16)
            result[pl.ds(first, GROUP), :, cols] = packed.reshape(GROUP, TILE, tail)

        @pl.loop(0, GROUP)
        def _(i):
            @pl.when(first + i < n - 1)
            def _():
                inbound(first + i).start()

    mine = pltpu.make_async_copy(result.at[n - 1], returned.at[n - 1], local_sem.at[1])
    mine.start()
    mine.wait()

    def collect(first):
        @pl.loop(0, GROUP)
        def _(i):
            @pl.when(first + i < n - 1)
            def _():
                inbound(first + i).wait_recv()

    collect(0)
    unpack(0, True)

    @pl.loop(1, n // GROUP)
    def _(g):
        collect(g * GROUP)
        unpack(g * GROUP, False)

    @pl.loop(0, n - 1)
    def _(k):
        outbound(k).wait_send()
        inbound(k).wait_send()


def fused(tokens, routed, slot, w_gate, w_up, w_down, pairs, eps, cap):
    n = pairs * eps
    tok_rows, depth = tokens.shape
    ff = w_gate.shape[2]
    spare = TILE - cap
    parts = cap // spare
    tail = depth * spare // TILE
    width = depth - tail

    rest_key = jnp.where(
        slot[None, :] // spare == jnp.arange(parts)[:, None],
        (routed * TILE + cap + slot % spare)[None, :],
        -1,
    )
    keys = jnp.concatenate([(routed * TILE + slot)[None, :], rest_key], axis=0)

    vmem = pl.BlockSpec(memory_space=pltpu.VMEM)
    hbm = pl.BlockSpec(memory_space=pl.ANY)
    bf16 = jnp.bfloat16
    parcels = pltpu.VMEM((n, TILE, width), bf16)
    head, ends = pl.pallas_call(
        functools.partial(exchange_ffn, pairs, eps, cap),
        out_shape=[
            jax.ShapeDtypeStruct((tok_rows, width), bf16),
            jax.ShapeDtypeStruct((tok_rows, tail), bf16),
        ],
        in_specs=[vmem, vmem, hbm, hbm, hbm, hbm],
        out_specs=[vmem, vmem],
        scratch_shapes=[
            pltpu.VMEM((tok_rows, depth), bf16),
            parcels,
            parcels,
            parcels,
            parcels,
            pltpu.VMEM((depth, ff), bf16),
            pltpu.VMEM((depth, ff), bf16),
            pltpu.VMEM((ff, depth), bf16),
            pltpu.VMEM((GROUP * TILE, ff), bf16),
            pltpu.VMEM((GROUP * TILE, tail), bf16),
            pltpu.SemaphoreType.DMA((1,)),
            pltpu.SemaphoreType.DMA((3,)),
            pltpu.SemaphoreType.DMA((2,)),
            pltpu.SemaphoreType.DMA((n,)),
            pltpu.SemaphoreType.DMA((n,)),
            pltpu.SemaphoreType.DMA((n,)),
            pltpu.SemaphoreType.DMA((n,)),
        ],
        compiler_params=pltpu.CompilerParams(
            collective_id=0, has_side_effects=True, vmem_limit_bytes=56 * 1024 * 1024
        ),
        name="exchange_ffn",
    )(keys, keys.T, tokens, w_gate, w_up, w_down)
    return jnp.concatenate([head, ends], axis=1)


def plain(tokens, routed, slot, w_gate, w_up, w_down, experts, capacity):
    position = routed * capacity + slot
    outgoing = (
        jnp.zeros((experts * capacity, tokens.shape[1]), jnp.bfloat16).at[position].set(tokens)
    )
    parcel = lax.all_to_all(
        outgoing.reshape(experts, capacity, outgoing.shape[1]),
        ("pair", "ep"), split_axis=0, concat_axis=0, tiled=True,
    )
    flat_rows = parcel.reshape(experts * capacity, parcel.shape[2])
    gate_proj = dot(flat_rows, w_gate[0])
    up_proj = dot(flat_rows, w_up[0])
    hidden = (jax.nn.silu(gate_proj) * up_proj).astype(jnp.bfloat16)
    result = dot(hidden, w_down[0]).astype(jnp.bfloat16)
    returned = lax.all_to_all(
        result.reshape(experts, capacity, result.shape[1]),
        ("pair", "ep"), split_axis=0, concat_axis=0, tiled=True,
    )
    return jnp.take(returned.reshape(experts * capacity, -1), position, axis=0)


BLOCK = 8


def near_ffn(
    pairs, eps, spill, keys_hbm, tok_hbm, gate_hbm, up_hbm, down_hbm, total, flag_hbm,
    tok, send_b, recv_b, res_b, ret_b, send_x, recv_x, res_x, ret_x, send_s, recv_s, res_s, ret_s,
    keys_ref, note, opinion, verdict, notes, gate, up, down, rows_x, hidden,
    load_sem, w_sem, ssem, rsem,
):
    n = pairs * eps
    near = n // 2
    line = eps // 2
    pair, ep = lax.axis_index("pair"), lax.axis_index("ep")
    rows_y = line // 2
    quarter = near // 2
    side = ep // line
    spot = lax.rem(ep % line + rows_y * (1 - side), line)
    outer, row_y = spot // rows_y, spot % rows_y
    tok_rows, depth = tok.shape
    mid = depth // 2
    ff = hidden.shape[1]
    extra = BLOCK // 2
    bf16, f32, i32 = jnp.bfloat16, jnp.float32, jnp.int32
    none = -4 * n * TILE
    wide = 512

    def peer(k, sign):
        i = k % near
        m = (i % quarter + 1) % quarter
        p = lax.rem(pair + pairs + sign * (m % pairs), pairs)
        y = lax.rem(row_y + rows_y + sign * (m // pairs), rows_y)
        there = lax.rem(side + 1 - k // near, 2)
        plane = lax.rem(outer + 1 - i // quarter + 1 - there, 2)
        return p, there * line + plane * rows_y + y

    key_load = pltpu.make_async_copy(keys_hbm, keys_ref, load_sem.at[0])
    key_load.start()
    tok_load = pltpu.make_async_copy(tok_hbm, tok, load_sem.at[1])
    tok_load.start()
    barrier = pltpu.get_barrier_semaphore()

    @pl.loop(0, n - 1)
    def _(k):
        pl.semaphore_signal(barrier, inc=1, device_id=peer(k, 1), device_id_type=MESH)

    loads = [
        pltpu.make_async_copy(src.at[0], dst, w_sem.at[i])
        for i, (src, dst) in enumerate(((gate_hbm, gate), (up_hbm, up), (down_hbm, down)))
    ]

    groups = {
        "far": (send_b, recv_b, 0, quarter),
        "far_too": (send_b, recv_b, quarter, near),
        "close": (send_b, recv_b, near, n - 1),
        "extra": (send_x, recv_x, 0, near - 1),
        "spill": (send_s, recv_s, 0, spill),
        "back_far": (res_b, ret_b, 0, quarter),
        "back_far_too": (res_b, ret_b, quarter, near),
        "back_close": (res_b, ret_b, near, n - 1),
        "back_extra": (res_x, ret_x, 0, near - 1),
        "back_spill": (res_s, ret_s, 0, spill),
    }
    ports = {name: i for i, name in enumerate(groups)}

    def remote(at, src, dst, to):
        return pltpu.make_async_remote_copy(
            src_ref=src, dst_ref=dst, send_sem=ssem.at[at], recv_sem=rsem.at[at],
            device_id=to, device_id_type=MESH,
        )

    mirror = peer(near - 1, 1)

    def go(name, turn=0):
        src, dst, low, high = groups[name]
        if src.shape[0] == spill:
            remote(ports[name], src, dst, mirror).start()
            return
        sign = -1 if name[:4] == "back" else 1
        skip = near if src.shape[0] == near else 0

        @pl.loop(0, high - low)
        def _(i):
            k = low + i + turn * quarter
            remote(ports[name] + turn, src.at[k], dst.at[k], peer(k + skip, sign)).start()

    def group(name, turn=0):
        src, dst, low, high = groups[name]
        part = pl.ds(low + turn * quarter, high - low)
        return remote(ports[name] + turn, src.at[part], dst.at[part], mirror)

    inner = 1 - outer
    last = len(groups)
    tell = remote(last, note, notes.at[near], mirror)

    def vote(k):
        return remote(last + 1, opinion, notes.at[k], peer(k + near, 1))

    votes = remote(last + 1, notes.at[pl.ds(0, near - 1)], notes.at[pl.ds(0, near - 1)], mirror)

    def iota(shape, axis):
        return lax.broadcasted_iota(i32, shape, axis)

    def one_hot(mask):
        return jnp.where(mask, 1.0, 0.0).astype(bf16)

    expert = iota((n, 128), 0)
    order = jnp.zeros((n, 128), i32)
    for k in range(n):
        p, e = peer(k, 1) if k < n - 1 else (pair, ep)
        order = jnp.where(expert == p * eps + e, k, order)
    order = order.astype(f32)
    key_load.wait()
    routed = keys_ref[...]
    which = iota((n, tok_rows), 0)
    chosen = jnp.where(which == routed, 1.0, 0.0)
    earlier = one_hot(iota((tok_rows, tok_rows), 0) < iota((tok_rows, tok_rows), 1))
    before = dot(chosen.astype(bf16), earlier)
    load_of = jnp.sum(chosen, axis=1, keepdims=True)
    over = jnp.where(order < near, jnp.maximum(load_of - BLOCK, 0.0), 0.0)
    ahead = jnp.where(which < routed, over[:, 0:1], 0.0)
    first = jnp.sum(ahead, axis=0, keepdims=True).astype(i32)
    rank = jnp.sum(chosen * order[:, 0:1], axis=0, keepdims=True).astype(i32)
    slot = jnp.sum(chosen * before, axis=0, keepdims=True).astype(i32)
    far = rank < near
    direct = slot < BLOCK
    spot_s = first + slot - BLOCK
    spilled = far & (slot >= BLOCK)
    spill_key = jnp.where(spilled, spot_s, none)

    def split(at, chunk):
        return pl.ds(pl.multiple_of(at + chunk * wide, wide), wide)

    def weave(left, right, count):
        left = left.reshape(count, BLOCK, wide)
        right = right.reshape(count, BLOCK, wide)
        return jnp.concatenate([left, right], axis=1).astype(bf16)

    tok_load.wait()
    for load in loads:
        load.start()

    spill_hot = one_hot(spill_key == iota((spill * BLOCK, tok_rows), 0))

    @pl.loop(0, mid // wide)
    def _(c):
        left = dot(spill_hot, tok[:, split(0, c)])
        right = dot(spill_hot, tok[:, split(mid, c)])
        send_s[:, :, split(0, c)] = weave(left, right, spill)

    pl.semaphore_wait(barrier, n - 1)
    go("spill")

    far_key = jnp.where(far & direct, rank * BLOCK + slot, none)
    beyond = jnp.where(direct, slot, near * BLOCK + slot - BLOCK)
    close_key = jnp.where(far, none, (rank - near) * BLOCK + beyond)
    pack_b = jnp.where(direct, rank * TILE + slot, none)
    pack_x = jnp.where(direct | far, none, (rank - near) * TILE + slot - BLOCK)
    pack_s = jnp.where(spilled, spot_s // BLOCK * TILE + spot_s % BLOCK, none)
    home = rank * TILE + extra + slot - BLOCK + 1
    lines = jnp.concatenate([pack_b, pack_x, pack_s, home, pack_b, pack_b, pack_b, pack_b], axis=0)
    cols = jnp.transpose(lines.astype(f32)).astype(i32)
    col_b, col_x, col_s, col_h = (cols[:, i:i + 1] for i in range(4))
    lane = iota((tok_rows, 128), 1)
    codes = jnp.where(col_s == lane, col_h, 0) + jnp.where(col_s + BLOCK == lane, col_h + BLOCK, 0)
    codes = jnp.sum(codes.astype(f32), axis=0, keepdims=True)
    excess = jnp.sum(over[:, 0:1], axis=0, keepdims=True) > spill * BLOCK
    excess = jnp.where(excess, 1.0, 0.0)
    note[...] = jnp.where(iota((1, 128), 1) == 127, excess, codes)

    tell.start()
    far_hot = one_hot(far_key == iota((near * BLOCK, tok_rows), 0))

    @pl.loop(0, mid // wide)
    def _(c):
        left = dot(far_hot, tok[:, split(0, c)])
        right = dot(far_hot, tok[:, split(mid, c)])
        send_b[pl.ds(0, near), :, split(0, c)] = weave(left, right, near)

    close_hot = one_hot(close_key == iota((2 * near * BLOCK, tok_rows), 0))

    @pl.loop(0, mid // wide)
    def _(c):
        left = dot(close_hot, tok[:, split(0, c)])
        right = dot(close_hot, tok[:, split(mid, c)])
        body = near * BLOCK
        send_b[pl.ds(near, near), :, split(0, c)] = weave(left[:body], right[:body], near)
        send_x[:, :, split(0, c)] = weave(left[body:], right[body:], near)

    @pl.when(inner == 1)
    def _():
        go("far", inner)
        go("far", outer)

    go("close")

    recv_b[n - 1] = send_b[n - 1]

    tell.wait_recv()
    group("spill").wait_recv()
    code = notes[near]
    depth_s = spill * TILE
    placed = code[:, :depth_s].astype(i32) - 1
    place_hot = one_hot(placed == iota((near * TILE, depth_s), 0))

    @pl.loop(0, mid // wide)
    def _(c):
        moved = dot(place_hot, recv_s[:, :, split(0, c)].reshape(depth_s, wide))
        mine = send_x[:, :, split(0, c)].reshape(near * TILE, wide).astype(f32)
        send_x[:, :, split(0, c)] = (mine + moved).astype(bf16).reshape(near, TILE, wide)

    go("extra")

    @pl.when(outer == 1)
    def _():
        go("far", inner)
        go("far", outer)

    recv_x[near - 1] = send_x[near - 1]

    opinion[...] = jnp.maximum(note[...], code)

    @pl.loop(0, near - 1)
    def _(k):
        vote(k).start()

    diagonal = iota((depth_s, 128), 0) == iota((depth_s, 128), 1)
    wanted = jnp.sum(jnp.where(diagonal, code, 0.0), axis=1, keepdims=True).astype(i32) - 1
    fetch_hot = one_hot(wanted == iota((depth_s, near * TILE), 1))

    for load in loads:
        load.wait()

    def ffn(arrived, result, base, count):
        rows = count * BLOCK

        @pl.loop(0, mid // wide)
        def _(c):
            piece = arrived[pl.ds(base, count), :, split(0, c)].astype(f32)
            rows_x[:rows, split(0, c)] = piece[:, :BLOCK].reshape(rows, wide).astype(bf16)
            rows_x[:rows, split(mid, c)] = piece[:, BLOCK:].reshape(rows, wide).astype(bf16)

        step = 256

        @pl.loop(0, ff // step)
        def _(f):
            at = pl.ds(pl.multiple_of(f * step, step), step)
            g_out = dot(rows_x[:rows, :], gate[:, at])
            u_out = dot(rows_x[:rows, :], up[:, at])
            hidden[:rows, at] = (jax.nn.silu(g_out) * u_out).astype(bf16)

        @pl.loop(0, mid // wide)
        def _(c):
            left = dot(hidden[:rows, :], down[:, split(0, c)])
            right = dot(hidden[:rows, :], down[:, split(mid, c)])
            result[pl.ds(base, count), :, split(0, c)] = weave(left, right, count)

    def unpack(col, returned, base, count, start):
        depth_k = count * TILE
        at = iota((tok_rows, depth_k), 1) + base * TILE
        left_hot = one_hot(col == at)
        right_hot = one_hot(col + BLOCK == at)

        @pl.loop(0, mid // wide)
        def _(c):
            piece = returned[pl.ds(base, count), :, split(0, c)].reshape(depth_k, wide)
            for hot, half in ((left_hot, 0), (right_hot, mid)):
                got = dot(hot, piece).astype(bf16)
                total[:, split(half, c)] = got if start else total[:, split(half, c)] + got

    group("close").wait_recv()
    ffn(recv_b, res_b, near, near)
    go("back_close")
    ret_b[n - 1] = res_b[n - 1]
    group("extra").wait_recv()
    ffn(recv_x, res_x, 0, near)
    go("back_extra")
    ret_x[near - 1] = res_x[near - 1]
    for turn in (inner, outer):
        group("far", turn).wait_recv()
        ffn(recv_b, res_b, turn * quarter, quarter)
        go("back_far", turn)

    for name in ("spill", "far", "far_too", "close", "extra"):
        group(name).wait_send()
    tell.wait_send()
    votes.wait_send()
    votes.wait_recv()
    worst = jnp.maximum(jnp.max(notes[pl.ds(0, near - 1)], axis=0), opinion[...])
    worst = jnp.where(iota((1, 128), 1) == 127, worst, 0.0)
    verdict[...] = jnp.max(worst, axis=1, keepdims=True)
    report = pltpu.make_async_copy(verdict, flag_hbm, load_sem.at[0])
    report.start()
    group("back_extra").wait_recv()

    @pl.loop(0, mid // wide)
    def _(c):
        piece = ret_x[:, :, split(0, c)].reshape(near * TILE, wide)
        res_s[:, :, split(0, c)] = dot(fetch_hot, piece).astype(bf16).reshape(spill, TILE, wide)

    go("back_spill")
    unpack(col_x, ret_x, 0, near, True)
    group("back_close").wait_recv()
    unpack(col_b, ret_b, near, near, False)
    def far(turn):
        group("back_far", turn).wait_recv()
        unpack(col_b, ret_b, turn * quarter, quarter, False)

    def relayed(when):
        @pl.when(outer == when)
        def _():
            group("back_spill").wait_recv()
            unpack(col_s, ret_s, 0, spill, False)

    far(inner)
    relayed(1)
    far(outer)
    relayed(0)
    for name in ("back_close", "back_far", "back_far_too", "back_extra", "back_spill"):
        group(name).wait_send()
    report.wait()


def spilling(tokens, routed, w_gate, w_up, w_down, pairs, eps):
    n = pairs * eps
    near = n // 2
    tok_rows, depth = tokens.shape
    ff = w_gate.shape[2]
    spill = 3
    bf16, f32 = jnp.bfloat16, jnp.float32
    vmem = pl.BlockSpec(memory_space=pltpu.VMEM)
    hbm = pl.BlockSpec(memory_space=pl.ANY)
    dma = pltpu.SemaphoreType.DMA

    def blocks(count):
        return pltpu.VMEM((count, TILE, depth // 2), bf16)

    return pl.pallas_call(
        functools.partial(near_ffn, pairs, eps, spill),
        out_shape=[
            jax.ShapeDtypeStruct((tok_rows, depth), bf16),
            jax.ShapeDtypeStruct((1, 1), f32),
        ],
        in_specs=[hbm, hbm, hbm, hbm, hbm],
        out_specs=[vmem, hbm],
        scratch_shapes=[
            pltpu.VMEM((tok_rows, depth), bf16),
            *[blocks(n)] * 4,
            *[blocks(near)] * 4,
            *[blocks(spill)] * 4,
            pltpu.VMEM((1, tok_rows), jnp.int32),
            pltpu.VMEM((1, 128), f32),
            pltpu.VMEM((1, 128), f32),
            pltpu.VMEM((1, 1), f32),
            pltpu.VMEM((near + 1, 1, 128), f32),
            pltpu.VMEM((depth, ff), bf16),
            pltpu.VMEM((depth, ff), bf16),
            pltpu.VMEM((ff, depth), bf16),
            pltpu.VMEM((near * BLOCK, depth), bf16),
            pltpu.VMEM((near * BLOCK, ff), bf16),
            dma((2,)), dma((3,)), dma((12,)), dma((12,)),
        ],
        compiler_params=pltpu.CompilerParams(
            collective_id=1, has_side_effects=True, vmem_limit_bytes=56 * 1024 * 1024
        ),
        name="near_ffn",
    )(routed.reshape(1, tok_rows), tokens, w_gate, w_up, w_down)


def dispatch(tokens, routed, w_gate, w_up, w_down, pairs, eps):
    experts = pairs * eps
    tok_rows, depth = tokens.shape
    cap = tok_rows // experts + tok_rows // (2 * experts)
    onehot = (routed[:, None] == jnp.arange(experts, dtype=jnp.int32)[None, :]).astype(jnp.float32)
    order = jnp.arange(tok_rows)
    earlier = (order[:, None] > order[None, :]).astype(jnp.bfloat16)
    before = dot(earlier, onehot.astype(jnp.bfloat16))
    slot = jnp.sum(before * onehot, axis=1).astype(jnp.int32)
    spare = TILE - cap
    packs = 0 < spare <= cap and cap % spare == 0 and (depth * spare) % (TILE * 256) == 0
    if packs and experts % GROUP == 0 and w_gate.shape[2] % 256 == 0:
        return fused(tokens, routed, slot, w_gate, w_up, w_down, pairs, eps, cap)
    return plain(tokens, routed, slot, w_gate, w_up, w_down, experts, cap)


def shards(tokens, expert_of, w_gate, w_up, w_down):
    pairs = lax.axis_size("pair")
    eps = lax.axis_size("ep")
    experts = pairs * eps
    tok_rows, depth = tokens.shape
    routed = expert_of[:, 0]
    whole = (tokens, routed, w_gate, w_up, w_down)
    even = tok_rows == BLOCK * experts and eps % 4 == 0 and experts % (2 * GROUP) == 0
    if not (even and depth % 1024 == 0 and w_gate.shape[2] % 256 == 0):
        return dispatch(*whole, pairs, eps)
    result, flag = spilling(*whole, pairs, eps)
    return lax.cond(
        flag[0, 0] > 0,
        lambda: dispatch(*whole, pairs, eps),
        lambda: result,
    )


def solution(mesh):
    spec2 = P(("pair", "ep"), None)
    spec3 = P(("pair", "ep"), None, None)
    return jax.shard_map(
        shards,
        mesh=mesh,
        in_specs=(spec2, spec2, spec3, spec3, spec3),
        out_specs=spec2,
        check_vma=False,
    )
```

```python
import functools

import jax
import jax.numpy as jnp
from jax import lax
from jax.experimental import pallas as pl
from jax.experimental.pallas import tpu as pltpu
from jax.sharding import PartitionSpec as P

MESH = pl.DeviceIdType.MESH
TILE = 16
GROUP = 8


def dot(a, b):
    return jnp.dot(a, b, preferred_element_type=jnp.float32)


def exchange_ffn(
    pairs, eps, cap, row_keys, col_keys, tok_hbm, gate_hbm, up_hbm, down_hbm, head_ref, ends_ref,
    tok, outgoing, recv, result, returned, gate, up, down, hidden, rest,
    tok_sem, w_sem, local_sem, send1, recv1, send2, recv2,
):
    n = pairs * eps
    pair, ep = lax.axis_index("pair"), lax.axis_index("ep")
    tok_rows = tok.shape[0]
    width = recv.shape[2]
    tail = rest.shape[1]
    parts = cap // (TILE - cap)
    spare = TILE - cap
    rows = GROUP * TILE
    bf16 = jnp.bfloat16

    def shift(k):
        i = k // pairs
        de = (eps // 2 + ((i + 1) // 2) * (2 * ((i + 1) % 2) - 1) + eps) % eps
        return (k + 1) % pairs, de

    def target(k):
        dp, de = shift(k)
        return lax.rem(pair + dp, pairs), lax.rem(ep + de, eps)

    def origin(k):
        dp, de = shift(k)
        return lax.rem(pair + pairs - dp, pairs), lax.rem(ep + eps - de, eps)

    tok_load = pltpu.make_async_copy(tok_hbm, tok, tok_sem.at[0])
    tok_load.start()

    barrier = pltpu.get_barrier_semaphore()

    @pl.loop(0, n - 1)
    def _(k):
        p, e = target(k)
        pl.semaphore_signal(barrier, inc=1, device_id=(p, e), device_id_type=MESH)

    loads = [
        pltpu.make_async_copy(src.at[0], dst, w_sem.at[i])
        for i, (src, dst) in enumerate(((gate_hbm, gate), (up_hbm, up), (down_hbm, down)))
    ]
    for load in loads:
        load.start()

    def outbound(k):
        p, e = target(k)
        return pltpu.make_async_remote_copy(
            src_ref=outgoing.at[k],
            dst_ref=recv.at[k],
            send_sem=send1.at[k],
            recv_sem=recv1.at[k],
            device_id=(p, e),
            device_id_type=MESH,
        )

    def inbound(k):
        p, e = origin(k)
        return pltpu.make_async_remote_copy(
            src_ref=result.at[k],
            dst_ref=returned.at[k],
            send_sem=send2.at[k],
            recv_sem=recv2.at[k],
            device_id=(p, e),
            device_id_type=MESH,
        )

    def row_ids(first, shape, axis):
        at = lax.broadcasted_iota(jnp.int32, shape, axis)
        base = jnp.zeros(shape, jnp.int32)
        for i in range(GROUP):
            p, e = target(first + i)
            base = jnp.where(at // TILE == i, (p * eps + e) * TILE, base)
        return base + at % TILE

    def one_hot(mask):
        return mask.astype(jnp.float32).astype(bf16)

    def pack(first):
        ids = row_ids(first, (rows, tok_rows), 0)
        main = one_hot(row_keys[0:1, :] == ids)
        for j in range(parts):
            cols = pl.ds(j * tail, tail)
            ends = one_hot(row_keys[j + 1:j + 2, :] == ids)
            piece = dot(main, tok[:, cols]) + dot(ends, tok[:, width:])
            outgoing[pl.ds(first, GROUP), :, cols] = piece.astype(bf16).reshape(GROUP, TILE, tail)

    def unpack(first, start):
        ids = row_ids(first, (tok_rows, rows), 1)
        main = one_hot(col_keys[:, 0:1] == ids)
        ends = jnp.zeros((tok_rows, tail), jnp.float32)
        for j in range(parts):
            cols = pl.ds(j * tail, tail)
            piece = returned[pl.ds(first, GROUP), :, cols].reshape(rows, tail)
            head = dot(main, piece).astype(bf16)
            head_ref[:, cols] = head if start else head_ref[:, cols] + head
            ends = ends + dot(one_hot(col_keys[:, j + 1:j + 2] == ids), piece)
        ends = ends.astype(bf16)
        ends_ref[...] = ends if start else ends_ref[...] + ends

    def send(first):
        @pl.loop(0, GROUP)
        def _(i):
            @pl.when(first + i < n - 1)
            def _():
                outbound(first + i).start()

    tok_load.wait()
    pack(0)
    pl.semaphore_wait(barrier, n - 1)
    send(0)

    @pl.loop(1, n // GROUP)
    def _(g):
        pack(g * GROUP)
        send(g * GROUP)

    own = pltpu.make_async_copy(outgoing.at[n - 1], recv.at[n - 1], local_sem.at[0])
    own.start()
    for load in loads:
        load.wait()
    own.wait()

    r = lax.broadcasted_iota(jnp.int32, (rows, rows), 0)
    c = lax.broadcasted_iota(jnp.int32, (rows, rows), 1)
    same = (r // TILE) == (c // TILE)
    r, c = r % TILE, c % TILE

    def spreader(j):
        return one_hot(same & (r // spare == j) & (c == cap + r % spare))

    def folder(j):
        return one_hot(same & (r >= cap) & (c == spare * j + r - cap))

    body_row = (lax.broadcasted_iota(jnp.int32, (rows, 1), 0) % TILE) < cap
    step = 256

    @pl.loop(0, n // GROUP)
    def _(g):
        first = g * GROUP

        @pl.loop(0, GROUP)
        def _(i):
            @pl.when(first + i < n - 1)
            def _():
                outbound(first + i).wait_recv()

        block = recv.at[pl.ds(first, GROUP)]
        total = jnp.zeros((rows, tail), jnp.float32)
        for j in range(parts):
            piece = block[:, :, j * tail:(j + 1) * tail].reshape(rows, tail)
            total = total + dot(spreader(j), piece)
        rest[...] = total.astype(bf16)

        @pl.loop(0, hidden.shape[1] // step)
        def _(f):
            cols = pl.ds(pl.multiple_of(f * step, step), step)
            main = block[...].reshape(rows, width)
            g_out = dot(main, gate[:width, cols]) + dot(rest[...], gate[width:, cols])
            u_out = dot(main, up[:width, cols]) + dot(rest[...], up[width:, cols])
            hidden[:, cols] = (jax.nn.silu(g_out) * u_out).astype(bf16)

        rest[...] = dot(hidden[...], down[:, width:]).astype(bf16)
        for j in range(parts):
            cols = pl.ds(j * tail, tail)
            body = dot(hidden[...], down[:, cols])
            extra = dot(folder(j), rest[...])
            packed = jnp.where(body_row, body, extra).astype(bf16)
            result[pl.ds(first, GROUP), :, cols] = packed.reshape(GROUP, TILE, tail)

        @pl.loop(0, GROUP)
        def _(i):
            @pl.when(first + i < n - 1)
            def _():
                inbound(first + i).start()

    mine = pltpu.make_async_copy(result.at[n - 1], returned.at[n - 1], local_sem.at[1])
    mine.start()
    mine.wait()

    def collect(first):
        @pl.loop(0, GROUP)
        def _(i):
            @pl.when(first + i < n - 1)
            def _():
                inbound(first + i).wait_recv()

    collect(0)
    unpack(0, True)

    @pl.loop(1, n // GROUP)
    def _(g):
        collect(g * GROUP)
        unpack(g * GROUP, False)

    @pl.loop(0, n - 1)
    def _(k):
        outbound(k).wait_send()
        inbound(k).wait_send()


def fused(tokens, routed, slot, w_gate, w_up, w_down, pairs, eps, cap):
    n = pairs * eps
    tok_rows, depth = tokens.shape
    ff = w_gate.shape[2]
    spare = TILE - cap
    parts = cap // spare
    tail = depth * spare // TILE
    width = depth - tail

    rest_key = jnp.where(
        slot[None, :] // spare == jnp.arange(parts)[:, None],
        (routed * TILE + cap + slot % spare)[None, :],
        -1,
    )
    keys = jnp.concatenate([(routed * TILE + slot)[None, :], rest_key], axis=0)

    vmem = pl.BlockSpec(memory_space=pltpu.VMEM)
    hbm = pl.BlockSpec(memory_space=pl.ANY)
    bf16 = jnp.bfloat16
    parcels = pltpu.VMEM((n, TILE, width), bf16)
    head, ends = pl.pallas_call(
        functools.partial(exchange_ffn, pairs, eps, cap),
        out_shape=[
            jax.ShapeDtypeStruct((tok_rows, width), bf16),
            jax.ShapeDtypeStruct((tok_rows, tail), bf16),
        ],
        in_specs=[vmem, vmem, hbm, hbm, hbm, hbm],
        out_specs=[vmem, vmem],
        scratch_shapes=[
            pltpu.VMEM((tok_rows, depth), bf16),
            parcels,
            parcels,
            parcels,
            parcels,
            pltpu.VMEM((depth, ff), bf16),
            pltpu.VMEM((depth, ff), bf16),
            pltpu.VMEM((ff, depth), bf16),
            pltpu.VMEM((GROUP * TILE, ff), bf16),
            pltpu.VMEM((GROUP * TILE, tail), bf16),
            pltpu.SemaphoreType.DMA((1,)),
            pltpu.SemaphoreType.DMA((3,)),
            pltpu.SemaphoreType.DMA((2,)),
            pltpu.SemaphoreType.DMA((n,)),
            pltpu.SemaphoreType.DMA((n,)),
            pltpu.SemaphoreType.DMA((n,)),
            pltpu.SemaphoreType.DMA((n,)),
        ],
        compiler_params=pltpu.CompilerParams(
            collective_id=0, has_side_effects=True, vmem_limit_bytes=56 * 1024 * 1024
        ),
        name="exchange_ffn",
    )(keys, keys.T, tokens, w_gate, w_up, w_down)
    return jnp.concatenate([head, ends], axis=1)


def plain(tokens, routed, slot, w_gate, w_up, w_down, experts, capacity):
    position = routed * capacity + slot
    outgoing = (
        jnp.zeros((experts * capacity, tokens.shape[1]), jnp.bfloat16).at[position].set(tokens)
    )
    parcel = lax.all_to_all(
        outgoing.reshape(experts, capacity, outgoing.shape[1]),
        ("pair", "ep"), split_axis=0, concat_axis=0, tiled=True,
    )
    flat_rows = parcel.reshape(experts * capacity, parcel.shape[2])
    gate_proj = dot(flat_rows, w_gate[0])
    up_proj = dot(flat_rows, w_up[0])
    hidden = (jax.nn.silu(gate_proj) * up_proj).astype(jnp.bfloat16)
    result = dot(hidden, w_down[0]).astype(jnp.bfloat16)
    returned = lax.all_to_all(
        result.reshape(experts, capacity, result.shape[1]),
        ("pair", "ep"), split_axis=0, concat_axis=0, tiled=True,
    )
    return jnp.take(returned.reshape(experts * capacity, -1), position, axis=0)


BLOCK = 8


def near_ffn(
    pairs, eps, spill, keys_hbm, tok_hbm, gate_hbm, up_hbm, down_hbm, total, flag_hbm,
    tok, send_b, recv_b, res_b, ret_b, send_x, recv_x, res_x, ret_x, send_s, recv_s, res_s, ret_s,
    keys_ref, note, opinion, verdict, notes, gate, up, down, rows_x, hidden,
    load_sem, w_sem, ssem, rsem,
):
    n = pairs * eps
    near = n // 2
    line = eps // 2
    pair, ep = lax.axis_index("pair"), lax.axis_index("ep")
    rows_y = line // 2
    quarter = near // 2
    side = ep // line
    spot = lax.rem(ep % line + rows_y * (1 - side), line)
    outer, row_y = spot // rows_y, spot % rows_y
    tok_rows, depth = tok.shape
    mid = depth // 2
    ff = hidden.shape[1]
    extra = BLOCK // 2
    bf16, f32, i32 = jnp.bfloat16, jnp.float32, jnp.int32
    none = -4 * n * TILE
    wide = 512

    def peer(k, sign):
        i = k % near
        m = (i % quarter + 1) % quarter
        p = lax.rem(pair + pairs + sign * (m % pairs), pairs)
        y = lax.rem(row_y + rows_y + sign * (m // pairs), rows_y)
        there = lax.rem(side + 1 - k // near, 2)
        plane = lax.rem(outer + 1 - i // quarter + 1 - there, 2)
        return p, there * line + plane * rows_y + y

    barrier = pltpu.get_barrier_semaphore()
    for k in range(n - 1):
        pl.semaphore_signal(barrier, inc=1, device_id=peer(k, 1), device_id_type=MESH)

    key_load = pltpu.make_async_copy(keys_hbm, keys_ref, load_sem.at[0])
    key_load.start()
    tok_load = pltpu.make_async_copy(tok_hbm, tok, load_sem.at[1])
    tok_load.start()

    loads = [
        pltpu.make_async_copy(src.at[0], dst, w_sem.at[i])
        for i, (src, dst) in enumerate(((gate_hbm, gate), (up_hbm, up), (down_hbm, down)))
    ]

    groups = {
        "far": (send_b, recv_b, 0, quarter),
        "far_too": (send_b, recv_b, quarter, near),
        "close": (send_b, recv_b, near, n - 1),
        "extra": (send_x, recv_x, 0, near - 1),
        "spill": (send_s, recv_s, 0, spill),
        "back_far": (res_b, ret_b, 0, quarter),
        "back_far_too": (res_b, ret_b, quarter, near),
        "back_close": (res_b, ret_b, near, n - 1),
        "back_extra": (res_x, ret_x, 0, near - 1),
        "back_spill": (res_s, ret_s, 0, spill),
    }
    ports = {name: i for i, name in enumerate(groups)}

    def remote(at, src, dst, to):
        return pltpu.make_async_remote_copy(
            src_ref=src, dst_ref=dst, send_sem=ssem.at[at], recv_sem=rsem.at[at],
            device_id=to, device_id_type=MESH,
        )

    mirror = peer(near - 1, 1)

    def go(name, turn=0):
        src, dst, low, high = groups[name]
        if src.shape[0] == spill:
            remote(ports[name], src, dst, mirror).start()
            return
        sign = -1 if name[:4] == "back" else 1
        skip = near if src.shape[0] == near else 0

        @pl.loop(0, high - low)
        def _(i):
            k = low + i + turn * quarter
            remote(ports[name] + turn, src.at[k], dst.at[k], peer(k + skip, sign)).start()

    def group(name, turn=0):
        src, dst, low, high = groups[name]
        part = pl.ds(low + turn * quarter, high - low)
        return remote(ports[name] + turn, src.at[part], dst.at[part], mirror)

    inner = 1 - outer
    last = len(groups)
    tell = remote(last, note, notes.at[near], mirror)

    def vote(k):
        return remote(last + 1, opinion, notes.at[k], peer(k + near, 1))

    votes = remote(last + 1, notes.at[pl.ds(0, near - 1)], notes.at[pl.ds(0, near - 1)], mirror)

    def iota(shape, axis):
        return lax.broadcasted_iota(i32, shape, axis)

    def one_hot(mask):
        return jnp.where(mask, 1.0, 0.0).astype(bf16)

    expert = iota((n, 128), 0)
    order = jnp.zeros((n, 128), i32)
    for k in range(n):
        p, e = peer(k, 1) if k < n - 1 else (pair, ep)
        order = jnp.where(expert == p * eps + e, k, order)
    order = order.astype(f32)
    key_load.wait()
    routed = keys_ref[...]
    which = iota((n, tok_rows), 0)
    chosen = jnp.where(which == routed, 1.0, 0.0)
    earlier = one_hot(iota((tok_rows, tok_rows), 0) < iota((tok_rows, tok_rows), 1))
    before = dot(chosen.astype(bf16), earlier)
    load_of = jnp.sum(chosen, axis=1, keepdims=True)
    over = jnp.where(order < near, jnp.maximum(load_of - BLOCK, 0.0), 0.0)
    ahead = jnp.where(which < routed, over[:, 0:1], 0.0)
    first = jnp.sum(ahead, axis=0, keepdims=True).astype(i32)
    rank = jnp.sum(chosen * order[:, 0:1], axis=0, keepdims=True).astype(i32)
    slot = jnp.sum(chosen * before, axis=0, keepdims=True).astype(i32)
    far = rank < near
    direct = slot < BLOCK
    spot_s = first + slot - BLOCK
    spilled = far & (slot >= BLOCK)
    spill_key = jnp.where(spilled, spot_s, none)

    def split(at, chunk):
        return pl.ds(pl.multiple_of(at + chunk * wide, wide), wide)

    def weave(left, right, count):
        left = left.reshape(count, BLOCK, wide)
        right = right.reshape(count, BLOCK, wide)
        return jnp.concatenate([left, right], axis=1).astype(bf16)

    tok_load.wait()
    for load in loads:
        load.start()

    spill_hot = one_hot(spill_key == iota((spill * BLOCK, tok_rows), 0))

    @pl.loop(0, mid // wide)
    def _(c):
        left = dot(spill_hot, tok[:, split(0, c)])
        right = dot(spill_hot, tok[:, split(mid, c)])
        send_s[:, :, split(0, c)] = weave(left, right, spill)

    pl.semaphore_wait(barrier, n - 1)
    go("spill")

    far_key = jnp.where(far & direct, rank * BLOCK + slot, none)
    beyond = jnp.where(direct, slot, near * BLOCK + slot - BLOCK)
    close_key = jnp.where(far, none, (rank - near) * BLOCK + beyond)
    pack_b = jnp.where(direct, rank * TILE + slot, none)
    pack_x = jnp.where(direct | far, none, (rank - near) * TILE + slot - BLOCK)
    pack_s = jnp.where(spilled, spot_s // BLOCK * TILE + spot_s % BLOCK, none)
    home = rank * TILE + extra + slot - BLOCK + 1
    lines = jnp.concatenate([pack_b, pack_x, pack_s, home, pack_b, pack_b, pack_b, pack_b], axis=0)
    cols = jnp.transpose(lines.astype(f32)).astype(i32)
    col_b, col_x, col_s, col_h = (cols[:, i:i + 1] for i in range(4))
    lane = iota((tok_rows, 128), 1)
    codes = jnp.where(col_s == lane, col_h, 0) + jnp.where(col_s + BLOCK == lane, col_h + BLOCK, 0)
    codes = jnp.sum(codes.astype(f32), axis=0, keepdims=True)
    excess = jnp.sum(over[:, 0:1], axis=0, keepdims=True) > spill * BLOCK
    excess = jnp.where(excess, 1.0, 0.0)
    note[...] = jnp.where(iota((1, 128), 1) == 127, excess, codes)

    tell.start()
    far_hot = one_hot(far_key == iota((near * BLOCK, tok_rows), 0))

    @pl.loop(0, mid // wide)
    def _(c):
        left = dot(far_hot, tok[:, split(0, c)])
        right = dot(far_hot, tok[:, split(mid, c)])
        send_b[pl.ds(0, near), :, split(0, c)] = weave(left, right, near)

    close_hot = one_hot(close_key == iota((2 * near * BLOCK, tok_rows), 0))

    @pl.loop(0, mid // wide)
    def _(c):
        left = dot(close_hot, tok[:, split(0, c)])
        right = dot(close_hot, tok[:, split(mid, c)])
        body = near * BLOCK
        send_b[pl.ds(near, near), :, split(0, c)] = weave(left[:body], right[:body], near)
        send_x[:, :, split(0, c)] = weave(left[body:], right[body:], near)

    @pl.when(inner == 1)
    def _():
        go("far", inner)
        go("far", outer)

    go("close")

    recv_b[n - 1] = send_b[n - 1]

    tell.wait_recv()
    group("spill").wait_recv()
    code = notes[near]
    depth_s = spill * TILE
    placed = code[:, :depth_s].astype(i32) - 1
    place_hot = one_hot(placed == iota((near * TILE, depth_s), 0))

    @pl.loop(0, mid // wide)
    def _(c):
        moved = dot(place_hot, recv_s[:, :, split(0, c)].reshape(depth_s, wide))
        mine = send_x[:, :, split(0, c)].reshape(near * TILE, wide).astype(f32)
        send_x[:, :, split(0, c)] = (mine + moved).astype(bf16).reshape(near, TILE, wide)

    go("extra")

    @pl.when(outer == 1)
    def _():
        go("far", inner)
        go("far", outer)

    recv_x[near - 1] = send_x[near - 1]

    opinion[...] = jnp.maximum(note[...], code)

    @pl.loop(0, near - 1)
    def _(k):
        vote(k).start()

    diagonal = iota((depth_s, 128), 0) == iota((depth_s, 128), 1)
    wanted = jnp.sum(jnp.where(diagonal, code, 0.0), axis=1, keepdims=True).astype(i32) - 1
    fetch_hot = one_hot(wanted == iota((depth_s, near * TILE), 1))

    for load in loads:
        load.wait()

    def ffn(arrived, result, base, count):
        rows = count * BLOCK

        @pl.loop(0, mid // wide)
        def _(c):
            piece = arrived[pl.ds(base, count), :, split(0, c)].astype(f32)
            rows_x[:rows, split(0, c)] = piece[:, :BLOCK].reshape(rows, wide).astype(bf16)
            rows_x[:rows, split(mid, c)] = piece[:, BLOCK:].reshape(rows, wide).astype(bf16)

        step = 256

        @pl.loop(0, ff // step)
        def _(f):
            at = pl.ds(pl.multiple_of(f * step, step), step)
            g_out = dot(rows_x[:rows, :], gate[:, at])
            u_out = dot(rows_x[:rows, :], up[:, at])
            hidden[:rows, at] = (jax.nn.silu(g_out) * u_out).astype(bf16)

        @pl.loop(0, mid // wide)
        def _(c):
            left = dot(hidden[:rows, :], down[:, split(0, c)])
            right = dot(hidden[:rows, :], down[:, split(mid, c)])
            result[pl.ds(base, count), :, split(0, c)] = weave(left, right, count)

    def unpack(col, returned, base, count, start):
        depth_k = count * TILE
        at = iota((tok_rows, depth_k), 1) + base * TILE
        left_hot = one_hot(col == at)
        right_hot = one_hot(col + BLOCK == at)

        @pl.loop(0, mid // wide)
        def _(c):
            piece = returned[pl.ds(base, count), :, split(0, c)].reshape(depth_k, wide)
            for hot, half in ((left_hot, 0), (right_hot, mid)):
                got = dot(hot, piece).astype(bf16)
                total[:, split(half, c)] = got if start else total[:, split(half, c)] + got

    group("close").wait_recv()
    ffn(recv_b, res_b, near, near)
    go("back_close")
    ret_b[n - 1] = res_b[n - 1]
    group("extra").wait_recv()
    ffn(recv_x, res_x, 0, near)
    go("back_extra")
    ret_x[near - 1] = res_x[near - 1]
    for turn in (1, 0):
        group("far", turn).wait_recv()
        ffn(recv_b, res_b, turn * quarter, quarter)
        go("back_far", turn)

    for name in ("spill", "far", "far_too", "close", "extra"):
        group(name).wait_send()
    tell.wait_send()
    votes.wait_send()
    votes.wait_recv()
    worst = jnp.maximum(jnp.max(notes[pl.ds(0, near - 1)], axis=0), opinion[...])
    worst = jnp.where(iota((1, 128), 1) == 127, worst, 0.0)
    verdict[...] = jnp.max(worst, axis=1, keepdims=True)
    report = pltpu.make_async_copy(verdict, flag_hbm, load_sem.at[0])
    report.start()
    group("back_extra").wait_recv()

    @pl.loop(0, mid // wide)
    def _(c):
        piece = ret_x[:, :, split(0, c)].reshape(near * TILE, wide)
        res_s[:, :, split(0, c)] = dot(fetch_hot, piece).astype(bf16).reshape(spill, TILE, wide)

    go("back_spill")
    unpack(col_x, ret_x, 0, near, True)
    group("back_close").wait_recv()
    unpack(col_b, ret_b, near, near, False)
    def far(turn):
        group("back_far", turn).wait_recv()
        unpack(col_b, ret_b, turn * quarter, quarter, False)

    def relayed(when):
        @pl.when(outer == when)
        def _():
            group("back_spill").wait_recv()
            unpack(col_s, ret_s, 0, spill, False)

    relayed(1)
    far(1)
    far(0)
    relayed(0)
    for name in ("back_close", "back_far", "back_far_too", "back_extra", "back_spill"):
        group(name).wait_send()
    report.wait()


def spilling(tokens, routed, w_gate, w_up, w_down, pairs, eps):
    n = pairs * eps
    near = n // 2
    tok_rows, depth = tokens.shape
    ff = w_gate.shape[2]
    spill = 3
    bf16, f32 = jnp.bfloat16, jnp.float32
    vmem = pl.BlockSpec(memory_space=pltpu.VMEM)
    hbm = pl.BlockSpec(memory_space=pl.ANY)
    dma = pltpu.SemaphoreType.DMA

    def blocks(count):
        return pltpu.VMEM((count, TILE, depth // 2), bf16)

    return pl.pallas_call(
        functools.partial(near_ffn, pairs, eps, spill),
        out_shape=[
            jax.ShapeDtypeStruct((tok_rows, depth), bf16),
            jax.ShapeDtypeStruct((1, 1), f32),
        ],
        in_specs=[hbm, hbm, hbm, hbm, hbm],
        out_specs=[vmem, hbm],
        scratch_shapes=[
            pltpu.VMEM((tok_rows, depth), bf16),
            *[blocks(n)] * 4,
            *[blocks(near)] * 4,
            *[blocks(spill)] * 4,
            pltpu.VMEM((1, tok_rows), jnp.int32),
            pltpu.VMEM((1, 128), f32),
            pltpu.VMEM((1, 128), f32),
            pltpu.VMEM((1, 1), f32),
            pltpu.VMEM((near + 1, 1, 128), f32),
            pltpu.VMEM((depth, ff), bf16),
            pltpu.VMEM((depth, ff), bf16),
            pltpu.VMEM((ff, depth), bf16),
            pltpu.VMEM((near * BLOCK, depth), bf16),
            pltpu.VMEM((near * BLOCK, ff), bf16),
            dma((2,)), dma((3,)), dma((12,)), dma((12,)),
        ],
        compiler_params=pltpu.CompilerParams(
            collective_id=1, has_side_effects=True, vmem_limit_bytes=56 * 1024 * 1024
        ),
        name="near_ffn",
    )(routed.reshape(1, tok_rows), tokens, w_gate, w_up, w_down)


def dispatch(tokens, routed, w_gate, w_up, w_down, pairs, eps):
    experts = pairs * eps
    tok_rows, depth = tokens.shape
    cap = tok_rows // experts + tok_rows // (2 * experts)
    onehot = (routed[:, None] == jnp.arange(experts, dtype=jnp.int32)[None, :]).astype(jnp.float32)
    order = jnp.arange(tok_rows)
    earlier = (order[:, None] > order[None, :]).astype(jnp.bfloat16)
    before = dot(earlier, onehot.astype(jnp.bfloat16))
    slot = jnp.sum(before * onehot, axis=1).astype(jnp.int32)
    spare = TILE - cap
    packs = 0 < spare <= cap and cap % spare == 0 and (depth * spare) % (TILE * 256) == 0
    if packs and experts % GROUP == 0 and w_gate.shape[2] % 256 == 0:
        return fused(tokens, routed, slot, w_gate, w_up, w_down, pairs, eps, cap)
    return plain(tokens, routed, slot, w_gate, w_up, w_down, experts, cap)


def shards(tokens, expert_of, w_gate, w_up, w_down):
    pairs = lax.axis_size("pair")
    eps = lax.axis_size("ep")
    experts = pairs * eps
    tok_rows, depth = tokens.shape
    routed = expert_of[:, 0]
    whole = (tokens, routed, w_gate, w_up, w_down)
    even = tok_rows == BLOCK * experts and eps % 4 == 0 and experts % (2 * GROUP) == 0
    if not (even and depth % 1024 == 0 and w_gate.shape[2] % 256 == 0):
        return dispatch(*whole, pairs, eps)
    result, flag = spilling(*whole, pairs, eps)
    return lax.cond(
        flag[0, 0] > 0,
        lambda: dispatch(*whole, pairs, eps),
        lambda: result,
    )


def solution(mesh):
    spec2 = P(("pair", "ep"), None)
    spec3 = P(("pair", "ep"), None, None)
    return jax.shard_map(
        shards,
        mesh=mesh,
        in_specs=(spec2, spec2, spec3, spec3, spec3),
        out_specs=spec2,
        check_vma=False,
    )
```

```python
import functools

import jax
import jax.numpy as jnp
from jax import lax
from jax.experimental import pallas as pl
from jax.experimental.pallas import tpu as pltpu
from jax.sharding import PartitionSpec as P

MESH = pl.DeviceIdType.MESH
TILE = 16
GROUP = 8


def dot(a, b):
    return jnp.dot(a, b, preferred_element_type=jnp.float32)


def exchange_ffn(
    pairs, eps, cap, row_keys, col_keys, tok_hbm, gate_hbm, up_hbm, down_hbm, head_ref, ends_ref,
    tok, outgoing, recv, result, returned, gate, up, down, hidden, rest,
    tok_sem, w_sem, local_sem, send1, recv1, send2, recv2,
):
    n = pairs * eps
    pair, ep = lax.axis_index("pair"), lax.axis_index("ep")
    tok_rows = tok.shape[0]
    width = recv.shape[2]
    tail = rest.shape[1]
    parts = cap // (TILE - cap)
    spare = TILE - cap
    rows = GROUP * TILE
    bf16 = jnp.bfloat16

    def shift(k):
        i = k // pairs
        de = (eps // 2 + ((i + 1) // 2) * (2 * ((i + 1) % 2) - 1) + eps) % eps
        return (k + 1) % pairs, de

    def target(k):
        dp, de = shift(k)
        return lax.rem(pair + dp, pairs), lax.rem(ep + de, eps)

    def origin(k):
        dp, de = shift(k)
        return lax.rem(pair + pairs - dp, pairs), lax.rem(ep + eps - de, eps)

    tok_load = pltpu.make_async_copy(tok_hbm, tok, tok_sem.at[0])
    tok_load.start()

    barrier = pltpu.get_barrier_semaphore()

    @pl.loop(0, n - 1)
    def _(k):
        p, e = target(k)
        pl.semaphore_signal(barrier, inc=1, device_id=(p, e), device_id_type=MESH)

    loads = [
        pltpu.make_async_copy(src.at[0], dst, w_sem.at[i])
        for i, (src, dst) in enumerate(((gate_hbm, gate), (up_hbm, up), (down_hbm, down)))
    ]
    for load in loads:
        load.start()

    def outbound(k):
        p, e = target(k)
        return pltpu.make_async_remote_copy(
            src_ref=outgoing.at[k],
            dst_ref=recv.at[k],
            send_sem=send1.at[k],
            recv_sem=recv1.at[k],
            device_id=(p, e),
            device_id_type=MESH,
        )

    def inbound(k):
        p, e = origin(k)
        return pltpu.make_async_remote_copy(
            src_ref=result.at[k],
            dst_ref=returned.at[k],
            send_sem=send2.at[k],
            recv_sem=recv2.at[k],
            device_id=(p, e),
            device_id_type=MESH,
        )

    def row_ids(first, shape, axis):
        at = lax.broadcasted_iota(jnp.int32, shape, axis)
        base = jnp.zeros(shape, jnp.int32)
        for i in range(GROUP):
            p, e = target(first + i)
            base = jnp.where(at // TILE == i, (p * eps + e) * TILE, base)
        return base + at % TILE

    def one_hot(mask):
        return mask.astype(jnp.float32).astype(bf16)

    def pack(first):
        ids = row_ids(first, (rows, tok_rows), 0)
        main = one_hot(row_keys[0:1, :] == ids)
        for j in range(parts):
            cols = pl.ds(j * tail, tail)
            ends = one_hot(row_keys[j + 1:j + 2, :] == ids)
            piece = dot(main, tok[:, cols]) + dot(ends, tok[:, width:])
            outgoing[pl.ds(first, GROUP), :, cols] = piece.astype(bf16).reshape(GROUP, TILE, tail)

    def unpack(first, start):
        ids = row_ids(first, (tok_rows, rows), 1)
        main = one_hot(col_keys[:, 0:1] == ids)
        ends = jnp.zeros((tok_rows, tail), jnp.float32)
        for j in range(parts):
            cols = pl.ds(j * tail, tail)
            piece = returned[pl.ds(first, GROUP), :, cols].reshape(rows, tail)
            head = dot(main, piece).astype(bf16)
            head_ref[:, cols] = head if start else head_ref[:, cols] + head
            ends = ends + dot(one_hot(col_keys[:, j + 1:j + 2] == ids), piece)
        ends = ends.astype(bf16)
        ends_ref[...] = ends if start else ends_ref[...] + ends

    def send(first):
        @pl.loop(0, GROUP)
        def _(i):
            @pl.when(first + i < n - 1)
            def _():
                outbound(first + i).start()

    tok_load.wait()
    pack(0)
    pl.semaphore_wait(barrier, n - 1)
    send(0)

    @pl.loop(1, n // GROUP)
    def _(g):
        pack(g * GROUP)
        send(g * GROUP)

    own = pltpu.make_async_copy(outgoing.at[n - 1], recv.at[n - 1], local_sem.at[0])
    own.start()
    for load in loads:
        load.wait()
    own.wait()

    r = lax.broadcasted_iota(jnp.int32, (rows, rows), 0)
    c = lax.broadcasted_iota(jnp.int32, (rows, rows), 1)
    same = (r // TILE) == (c // TILE)
    r, c = r % TILE, c % TILE

    def spreader(j):
        return one_hot(same & (r // spare == j) & (c == cap + r % spare))

    def folder(j):
        return one_hot(same & (r >= cap) & (c == spare * j + r - cap))

    body_row = (lax.broadcasted_iota(jnp.int32, (rows, 1), 0) % TILE) < cap
    step = 256

    @pl.loop(0, n // GROUP)
    def _(g):
        first = g * GROUP

        @pl.loop(0, GROUP)
        def _(i):
            @pl.when(first + i < n - 1)
            def _():
                outbound(first + i).wait_recv()

        block = recv.at[pl.ds(first, GROUP)]
        total = jnp.zeros((rows, tail), jnp.float32)
        for j in range(parts):
            piece = block[:, :, j * tail:(j + 1) * tail].reshape(rows, tail)
            total = total + dot(spreader(j), piece)
        rest[...] = total.astype(bf16)

        @pl.loop(0, hidden.shape[1] // step)
        def _(f):
            cols = pl.ds(pl.multiple_of(f * step, step), step)
            main = block[...].reshape(rows, width)
            g_out = dot(main, gate[:width, cols]) + dot(rest[...], gate[width:, cols])
            u_out = dot(main, up[:width, cols]) + dot(rest[...], up[width:, cols])
            hidden[:, cols] = (jax.nn.silu(g_out) * u_out).astype(bf16)

        rest[...] = dot(hidden[...], down[:, width:]).astype(bf16)
        for j in range(parts):
            cols = pl.ds(j * tail, tail)
            body = dot(hidden[...], down[:, cols])
            extra = dot(folder(j), rest[...])
            packed = jnp.where(body_row, body, extra).astype(bf16)
            result[pl.ds(first, GROUP), :, cols] = packed.reshape(GROUP, TILE, tail)

        @pl.loop(0, GROUP)
        def _(i):
            @pl.when(first + i < n - 1)
            def _():
                inbound(first + i).start()

    mine = pltpu.make_async_copy(result.at[n - 1], returned.at[n - 1], local_sem.at[1])
    mine.start()
    mine.wait()

    def collect(first):
        @pl.loop(0, GROUP)
        def _(i):
            @pl.when(first + i < n - 1)
            def _():
                inbound(first + i).wait_recv()

    collect(0)
    unpack(0, True)

    @pl.loop(1, n // GROUP)
    def _(g):
        collect(g * GROUP)
        unpack(g * GROUP, False)

    @pl.loop(0, n - 1)
    def _(k):
        outbound(k).wait_send()
        inbound(k).wait_send()


def fused(tokens, routed, slot, w_gate, w_up, w_down, pairs, eps, cap):
    n = pairs * eps
    tok_rows, depth = tokens.shape
    ff = w_gate.shape[2]
    spare = TILE - cap
    parts = cap // spare
    tail = depth * spare // TILE
    width = depth - tail

    rest_key = jnp.where(
        slot[None, :] // spare == jnp.arange(parts)[:, None],
        (routed * TILE + cap + slot % spare)[None, :],
        -1,
    )
    keys = jnp.concatenate([(routed * TILE + slot)[None, :], rest_key], axis=0)

    vmem = pl.BlockSpec(memory_space=pltpu.VMEM)
    hbm = pl.BlockSpec(memory_space=pl.ANY)
    bf16 = jnp.bfloat16
    parcels = pltpu.VMEM((n, TILE, width), bf16)
    head, ends = pl.pallas_call(
        functools.partial(exchange_ffn, pairs, eps, cap),
        out_shape=[
            jax.ShapeDtypeStruct((tok_rows, width), bf16),
            jax.ShapeDtypeStruct((tok_rows, tail), bf16),
        ],
        in_specs=[vmem, vmem, hbm, hbm, hbm, hbm],
        out_specs=[vmem, vmem],
        scratch_shapes=[
            pltpu.VMEM((tok_rows, depth), bf16),
            parcels,
            parcels,
            parcels,
            parcels,
            pltpu.VMEM((depth, ff), bf16),
            pltpu.VMEM((depth, ff), bf16),
            pltpu.VMEM((ff, depth), bf16),
            pltpu.VMEM((GROUP * TILE, ff), bf16),
            pltpu.VMEM((GROUP * TILE, tail), bf16),
            pltpu.SemaphoreType.DMA((1,)),
            pltpu.SemaphoreType.DMA((3,)),
            pltpu.SemaphoreType.DMA((2,)),
            pltpu.SemaphoreType.DMA((n,)),
            pltpu.SemaphoreType.DMA((n,)),
            pltpu.SemaphoreType.DMA((n,)),
            pltpu.SemaphoreType.DMA((n,)),
        ],
        compiler_params=pltpu.CompilerParams(
            collective_id=0, has_side_effects=True, vmem_limit_bytes=56 * 1024 * 1024
        ),
        name="exchange_ffn",
    )(keys, keys.T, tokens, w_gate, w_up, w_down)
    return jnp.concatenate([head, ends], axis=1)


def plain(tokens, routed, slot, w_gate, w_up, w_down, experts, capacity):
    position = routed * capacity + slot
    outgoing = (
        jnp.zeros((experts * capacity, tokens.shape[1]), jnp.bfloat16).at[position].set(tokens)
    )
    parcel = lax.all_to_all(
        outgoing.reshape(experts, capacity, outgoing.shape[1]),
        ("pair", "ep"), split_axis=0, concat_axis=0, tiled=True,
    )
    flat_rows = parcel.reshape(experts * capacity, parcel.shape[2])
    gate_proj = dot(flat_rows, w_gate[0])
    up_proj = dot(flat_rows, w_up[0])
    hidden = (jax.nn.silu(gate_proj) * up_proj).astype(jnp.bfloat16)
    result = dot(hidden, w_down[0]).astype(jnp.bfloat16)
    returned = lax.all_to_all(
        result.reshape(experts, capacity, result.shape[1]),
        ("pair", "ep"), split_axis=0, concat_axis=0, tiled=True,
    )
    return jnp.take(returned.reshape(experts * capacity, -1), position, axis=0)


BLOCK = 8


def near_ffn(
    pairs, eps, spill, keys_hbm, tok_hbm, gate_hbm, up_hbm, down_hbm, total, flag_hbm,
    tok, send_b, recv_b, res_b, ret_b, send_x, recv_x, res_x, ret_x, send_s, recv_s, res_s, ret_s,
    keys_ref, note, opinion, verdict, notes, gate, up, down, rows_x, hidden,
    load_sem, w_sem, ssem, rsem,
):
    n = pairs * eps
    near = n // 2
    line = eps // 2
    pair, ep = lax.axis_index("pair"), lax.axis_index("ep")
    rows_y = line // 2
    quarter = near // 2
    side = ep // line
    spot = lax.rem(ep % line + rows_y * (1 - side), line)
    outer, row_y = spot // rows_y, spot % rows_y
    tok_rows, depth = tok.shape
    mid = depth // 2
    ff = hidden.shape[1]
    extra = BLOCK // 2
    bf16, f32, i32 = jnp.bfloat16, jnp.float32, jnp.int32
    none = -4 * n * TILE
    wide = 512

    def peer(k, sign):
        i = k % near
        m = (i % quarter + 1) % quarter
        p = lax.rem(pair + pairs + sign * (m % pairs), pairs)
        y = lax.rem(row_y + rows_y + sign * (m // pairs), rows_y)
        there = lax.rem(side + 1 - k // near, 2)
        plane = lax.rem(outer + 1 - i // quarter + 1 - there, 2)
        return p, there * line + plane * rows_y + y

    barrier = pltpu.get_barrier_semaphore()
    for k in range(n - 1):
        pl.semaphore_signal(barrier, inc=1, device_id=peer(k, 1), device_id_type=MESH)

    key_load = pltpu.make_async_copy(keys_hbm, keys_ref, load_sem.at[0])
    key_load.start()
    tok_load = pltpu.make_async_copy(tok_hbm, tok, load_sem.at[1])
    tok_load.start()

    loads = [
        pltpu.make_async_copy(src.at[0], dst, w_sem.at[i])
        for i, (src, dst) in enumerate(((gate_hbm, gate), (up_hbm, up), (down_hbm, down)))
    ]

    groups = {
        "far": (send_b, recv_b, 0, quarter),
        "far_too": (send_b, recv_b, quarter, near),
        "close": (send_b, recv_b, near, n - 1),
        "extra": (send_x, recv_x, 0, near - 1),
        "spill": (send_s, recv_s, 0, spill),
        "back_far": (res_b, ret_b, 0, quarter),
        "back_far_too": (res_b, ret_b, quarter, near),
        "back_close": (res_b, ret_b, near, n - 1),
        "back_extra": (res_x, ret_x, 0, near - 1),
        "back_spill": (res_s, ret_s, 0, spill),
    }
    ports = {name: i for i, name in enumerate(groups)}

    def remote(at, src, dst, to):
        return pltpu.make_async_remote_copy(
            src_ref=src, dst_ref=dst, send_sem=ssem.at[at], recv_sem=rsem.at[at],
            device_id=to, device_id_type=MESH,
        )

    mirror = peer(near - 1, 1)

    def go(name, turn=0):
        src, dst, low, high = groups[name]
        if src.shape[0] == spill:
            remote(ports[name], src, dst, mirror).start()
            return
        sign = -1 if name[:4] == "back" else 1
        skip = near if src.shape[0] == near else 0

        @pl.loop(0, high - low)
        def _(i):
            k = low + i + turn * quarter
            remote(ports[name] + turn, src.at[k], dst.at[k], peer(k + skip, sign)).start()

    def group(name, turn=0):
        src, dst, low, high = groups[name]
        part = pl.ds(low + turn * quarter, high - low)
        return remote(ports[name] + turn, src.at[part], dst.at[part], mirror)

    inner = 1 - outer
    last = len(groups)
    late = {"back_far": last + 2, "back_spill": last + 3}

    def lanes(j):
        return pl.ds(j * (mid // 2), mid // 2)

    def go_half(name, j):
        src, dst, low, high = groups[name]
        at = late[name] if j else ports[name]
        if src.shape[0] == spill:
            remote(at, src.at[:, :, lanes(j)], dst.at[:, :, lanes(j)], mirror).start()
            return

        @pl.loop(low, high)
        def _(k):
            remote(at, src.at[k, :, lanes(j)], dst.at[k, :, lanes(j)], peer(k, -1)).start()

    def half_group(name, j):
        src, dst, low, high = groups[name]
        part = pl.ds(low, high - low)
        at = late[name] if j else ports[name]
        return remote(at, src.at[part, :, lanes(j)], dst.at[part, :, lanes(j)], mirror)

    tell = remote(last, note, notes.at[near], mirror)

    def vote(k):
        return remote(last + 1, opinion, notes.at[k], peer(k + near, 1))

    votes = remote(last + 1, notes.at[pl.ds(0, near - 1)], notes.at[pl.ds(0, near - 1)], mirror)

    def iota(shape, axis):
        return lax.broadcasted_iota(i32, shape, axis)

    def one_hot(mask):
        return jnp.where(mask, 1.0, 0.0).astype(bf16)

    expert = iota((n, 128), 0)
    order = jnp.zeros((n, 128), i32)
    for k in range(n):
        p, e = peer(k, 1) if k < n - 1 else (pair, ep)
        order = jnp.where(expert == p * eps + e, k, order)
    order = order.astype(f32)
    key_load.wait()
    routed = keys_ref[...]
    which = iota((n, tok_rows), 0)
    chosen = jnp.where(which == routed, 1.0, 0.0)
    earlier = one_hot(iota((tok_rows, tok_rows), 0) < iota((tok_rows, tok_rows), 1))
    before = dot(chosen.astype(bf16), earlier)
    load_of = jnp.sum(chosen, axis=1, keepdims=True)
    over = jnp.where(order < near, jnp.maximum(load_of - BLOCK, 0.0), 0.0)
    ahead = jnp.where(which < routed, over[:, 0:1], 0.0)
    first = jnp.sum(ahead, axis=0, keepdims=True).astype(i32)
    rank = jnp.sum(chosen * order[:, 0:1], axis=0, keepdims=True).astype(i32)
    slot = jnp.sum(chosen * before, axis=0, keepdims=True).astype(i32)
    far = rank < near
    direct = slot < BLOCK
    spot_s = first + slot - BLOCK
    spilled = far & (slot >= BLOCK)
    spill_key = jnp.where(spilled, spot_s, none)

    def split(at, chunk):
        return pl.ds(pl.multiple_of(at + chunk * wide, wide), wide)

    def weave(left, right, count):
        left = left.reshape(count, BLOCK, wide)
        right = right.reshape(count, BLOCK, wide)
        return jnp.concatenate([left, right], axis=1).astype(bf16)

    tok_load.wait()
    for load in loads:
        load.start()

    spill_hot = one_hot(spill_key == iota((spill * BLOCK, tok_rows), 0))

    @pl.loop(0, mid // wide)
    def _(c):
        left = dot(spill_hot, tok[:, split(0, c)])
        right = dot(spill_hot, tok[:, split(mid, c)])
        send_s[:, :, split(0, c)] = weave(left, right, spill)

    pl.semaphore_wait(barrier, n - 1)
    go("spill")

    far_key = jnp.where(far & direct, rank * BLOCK + slot, none)
    beyond = jnp.where(direct, slot, near * BLOCK + slot - BLOCK)
    close_key = jnp.where(far, none, (rank - near) * BLOCK + beyond)
    pack_b = jnp.where(direct, rank * TILE + slot, none)
    pack_x = jnp.where(direct | far, none, (rank - near) * TILE + slot - BLOCK)
    pack_s = jnp.where(spilled, spot_s // BLOCK * TILE + spot_s % BLOCK, none)
    home = rank * TILE + extra + slot - BLOCK + 1
    lines = jnp.concatenate([pack_b, pack_x, pack_s, home, pack_b, pack_b, pack_b, pack_b], axis=0)
    cols = jnp.transpose(lines.astype(f32)).astype(i32)
    col_b, col_x, col_s, col_h = (cols[:, i:i + 1] for i in range(4))
    lane = iota((tok_rows, 128), 1)
    codes = jnp.where(col_s == lane, col_h, 0) + jnp.where(col_s + BLOCK == lane, col_h + BLOCK, 0)
    codes = jnp.sum(codes.astype(f32), axis=0, keepdims=True)
    excess = jnp.sum(over[:, 0:1], axis=0, keepdims=True) > spill * BLOCK
    excess = jnp.where(excess, 1.0, 0.0)
    note[...] = jnp.where(iota((1, 128), 1) == 127, excess, codes)

    tell.start()
    far_hot = one_hot(far_key == iota((near * BLOCK, tok_rows), 0))

    @pl.loop(0, mid // wide)
    def _(c):
        left = dot(far_hot, tok[:, split(0, c)])
        right = dot(far_hot, tok[:, split(mid, c)])
        send_b[pl.ds(0, near), :, split(0, c)] = weave(left, right, near)

    close_hot = one_hot(close_key == iota((2 * near * BLOCK, tok_rows), 0))

    @pl.loop(0, mid // wide)
    def _(c):
        left = dot(close_hot, tok[:, split(0, c)])
        right = dot(close_hot, tok[:, split(mid, c)])
        body = near * BLOCK
        send_b[pl.ds(near, near), :, split(0, c)] = weave(left[:body], right[:body], near)
        send_x[:, :, split(0, c)] = weave(left[body:], right[body:], near)

    @pl.when(inner == 1)
    def _():
        go("far", inner)
        go("far", outer)

    go("close")

    recv_b[n - 1] = send_b[n - 1]

    tell.wait_recv()
    group("spill").wait_recv()
    code = notes[near]
    depth_s = spill * TILE
    placed = code[:, :depth_s].astype(i32) - 1
    place_hot = one_hot(placed == iota((near * TILE, depth_s), 0))

    @pl.loop(0, mid // wide)
    def _(c):
        moved = dot(place_hot, recv_s[:, :, split(0, c)].reshape(depth_s, wide))
        mine = send_x[:, :, split(0, c)].reshape(near * TILE, wide).astype(f32)
        send_x[:, :, split(0, c)] = (mine + moved).astype(bf16).reshape(near, TILE, wide)

    go("extra")

    @pl.when(outer == 1)
    def _():
        go("far", inner)
        go("far", outer)

    recv_x[near - 1] = send_x[near - 1]

    opinion[...] = jnp.maximum(note[...], code)

    @pl.loop(0, near - 1)
    def _(k):
        vote(k).start()

    diagonal = iota((depth_s, 128), 0) == iota((depth_s, 128), 1)
    wanted = jnp.sum(jnp.where(diagonal, code, 0.0), axis=1, keepdims=True).astype(i32) - 1
    fetch_hot = one_hot(wanted == iota((depth_s, near * TILE), 1))

    for load in loads:
        load.wait()

    def ffn(arrived, result, base, count):
        rows = count * BLOCK

        @pl.loop(0, mid // wide)
        def _(c):
            piece = arrived[pl.ds(base, count), :, split(0, c)].astype(f32)
            rows_x[:rows, split(0, c)] = piece[:, :BLOCK].reshape(rows, wide).astype(bf16)
            rows_x[:rows, split(mid, c)] = piece[:, BLOCK:].reshape(rows, wide).astype(bf16)

        step = 256

        @pl.loop(0, ff // step)
        def _(f):
            at = pl.ds(pl.multiple_of(f * step, step), step)
            g_out = dot(rows_x[:rows, :], gate[:, at])
            u_out = dot(rows_x[:rows, :], up[:, at])
            hidden[:rows, at] = (jax.nn.silu(g_out) * u_out).astype(bf16)

        @pl.loop(0, mid // wide)
        def _(c):
            left = dot(hidden[:rows, :], down[:, split(0, c)])
            right = dot(hidden[:rows, :], down[:, split(mid, c)])
            result[pl.ds(base, count), :, split(0, c)] = weave(left, right, count)

    def unpack(col, returned, base, count, start, part=None):
        depth_k = count * TILE
        at = iota((tok_rows, depth_k), 1) + base * TILE
        left_hot = one_hot(col == at)
        right_hot = one_hot(col + BLOCK == at)
        chunks = mid // wide
        low, high = (0, chunks) if part is None else (part * chunks // 2, (part + 1) * chunks // 2)

        @pl.loop(low, high)
        def _(c):
            piece = returned[pl.ds(base, count), :, split(0, c)].reshape(depth_k, wide)
            for hot, half in ((left_hot, 0), (right_hot, mid)):
                got = dot(hot, piece).astype(bf16)
                total[:, split(half, c)] = got if start else total[:, split(half, c)] + got

    group("close").wait_recv()
    ffn(recv_b, res_b, near, near)
    go("back_close")
    ret_b[n - 1] = res_b[n - 1]
    group("extra").wait_recv()
    ffn(recv_x, res_x, 0, near)
    go("back_extra")
    ret_x[near - 1] = res_x[near - 1]
    for turn in (1, 0):
        group("far", turn).wait_recv()
        ffn(recv_b, res_b, turn * quarter, quarter)
        if turn:
            go("back_far", turn)
        else:
            go_half("back_far", 0)
            go_half("back_far", 1)

    for name in ("spill", "far", "far_too", "close", "extra"):
        group(name).wait_send()
    tell.wait_send()
    votes.wait_send()
    votes.wait_recv()
    worst = jnp.maximum(jnp.max(notes[pl.ds(0, near - 1)], axis=0), opinion[...])
    worst = jnp.where(iota((1, 128), 1) == 127, worst, 0.0)
    verdict[...] = jnp.max(worst, axis=1, keepdims=True)
    report = pltpu.make_async_copy(verdict, flag_hbm, load_sem.at[0])
    report.start()
    group("back_extra").wait_recv()

    @pl.loop(0, mid // wide)
    def _(c):
        piece = ret_x[:, :, split(0, c)].reshape(near * TILE, wide)
        res_s[:, :, split(0, c)] = dot(fetch_hot, piece).astype(bf16).reshape(spill, TILE, wide)

    go_half("back_spill", 0)
    go_half("back_spill", 1)
    unpack(col_x, ret_x, 0, near, True)
    group("back_close").wait_recv()
    unpack(col_b, ret_b, near, near, False)
    def relayed(when):
        @pl.when(outer == when)
        def _():
            for j in range(2):
                half_group("back_spill", j).wait_recv()
                unpack(col_s, ret_s, 0, spill, False, j)

    relayed(1)
    group("back_far", 1).wait_recv()
    unpack(col_b, ret_b, quarter, quarter, False)
    for j in range(2):
        half_group("back_far", j).wait_recv()
        unpack(col_b, ret_b, 0, quarter, False, j)
    relayed(0)
    for name in ("back_close", "back_far_too", "back_extra"):
        group(name).wait_send()
    for j in range(2):
        half_group("back_far", j).wait_send()
        half_group("back_spill", j).wait_send()
    report.wait()


def spilling(tokens, routed, w_gate, w_up, w_down, pairs, eps):
    n = pairs * eps
    near = n // 2
    tok_rows, depth = tokens.shape
    ff = w_gate.shape[2]
    spill = 3
    bf16, f32 = jnp.bfloat16, jnp.float32
    vmem = pl.BlockSpec(memory_space=pltpu.VMEM)
    hbm = pl.BlockSpec(memory_space=pl.ANY)
    dma = pltpu.SemaphoreType.DMA

    def blocks(count):
        return pltpu.VMEM((count, TILE, depth // 2), bf16)

    return pl.pallas_call(
        functools.partial(near_ffn, pairs, eps, spill),
        out_shape=[
            jax.ShapeDtypeStruct((tok_rows, depth), bf16),
            jax.ShapeDtypeStruct((1, 1), f32),
        ],
        in_specs=[hbm, hbm, hbm, hbm, hbm],
        out_specs=[vmem, hbm],
        scratch_shapes=[
            pltpu.VMEM((tok_rows, depth), bf16),
            *[blocks(n)] * 4,
            *[blocks(near)] * 4,
            *[blocks(spill)] * 4,
            pltpu.VMEM((1, tok_rows), jnp.int32),
            pltpu.VMEM((1, 128), f32),
            pltpu.VMEM((1, 128), f32),
            pltpu.VMEM((1, 1), f32),
            pltpu.VMEM((near + 1, 1, 128), f32),
            pltpu.VMEM((depth, ff), bf16),
            pltpu.VMEM((depth, ff), bf16),
            pltpu.VMEM((ff, depth), bf16),
            pltpu.VMEM((near * BLOCK, depth), bf16),
            pltpu.VMEM((near * BLOCK, ff), bf16),
            dma((2,)), dma((3,)), dma((14,)), dma((14,)),
        ],
        compiler_params=pltpu.CompilerParams(
            collective_id=1, has_side_effects=True, vmem_limit_bytes=56 * 1024 * 1024
        ),
        name="near_ffn",
    )(routed.reshape(1, tok_rows), tokens, w_gate, w_up, w_down)


def dispatch(tokens, routed, w_gate, w_up, w_down, pairs, eps):
    experts = pairs * eps
    tok_rows, depth = tokens.shape
    cap = tok_rows // experts + tok_rows // (2 * experts)
    onehot = (routed[:, None] == jnp.arange(experts, dtype=jnp.int32)[None, :]).astype(jnp.float32)
    order = jnp.arange(tok_rows)
    earlier = (order[:, None] > order[None, :]).astype(jnp.bfloat16)
    before = dot(earlier, onehot.astype(jnp.bfloat16))
    slot = jnp.sum(before * onehot, axis=1).astype(jnp.int32)
    spare = TILE - cap
    packs = 0 < spare <= cap and cap % spare == 0 and (depth * spare) % (TILE * 256) == 0
    if packs and experts % GROUP == 0 and w_gate.shape[2] % 256 == 0:
        return fused(tokens, routed, slot, w_gate, w_up, w_down, pairs, eps, cap)
    return plain(tokens, routed, slot, w_gate, w_up, w_down, experts, cap)


def shards(tokens, expert_of, w_gate, w_up, w_down):
    pairs = lax.axis_size("pair")
    eps = lax.axis_size("ep")
    experts = pairs * eps
    tok_rows, depth = tokens.shape
    routed = expert_of[:, 0]
    whole = (tokens, routed, w_gate, w_up, w_down)
    even = tok_rows == BLOCK * experts and eps % 4 == 0 and experts % (2 * GROUP) == 0
    if not (even and depth % 1024 == 0 and w_gate.shape[2] % 256 == 0):
        return dispatch(*whole, pairs, eps)
    result, flag = spilling(*whole, pairs, eps)
    return lax.cond(
        flag[0, 0] > 0,
        lambda: dispatch(*whole, pairs, eps),
        lambda: result,
    )


def solution(mesh):
    spec2 = P(("pair", "ep"), None)
    spec3 = P(("pair", "ep"), None, None)
    return jax.shard_map(
        shards,
        mesh=mesh,
        in_specs=(spec2, spec2, spec3, spec3, spec3),
        out_specs=spec2,
        check_vma=False,
    )
```

```python
import functools

import jax
import jax.numpy as jnp
from jax import lax
from jax.experimental import pallas as pl
from jax.experimental.pallas import tpu as pltpu
from jax.sharding import PartitionSpec as P

MESH = pl.DeviceIdType.MESH
TILE = 16
GROUP = 8


def dot(a, b):
    return jnp.dot(a, b, preferred_element_type=jnp.float32)


def exchange_ffn(
    pairs, eps, cap, row_keys, col_keys, tok_hbm, gate_hbm, up_hbm, down_hbm, head_ref, ends_ref,
    tok, outgoing, recv, result, returned, gate, up, down, hidden, rest,
    tok_sem, w_sem, local_sem, send1, recv1, send2, recv2,
):
    n = pairs * eps
    pair, ep = lax.axis_index("pair"), lax.axis_index("ep")
    tok_rows = tok.shape[0]
    width = recv.shape[2]
    tail = rest.shape[1]
    parts = cap // (TILE - cap)
    spare = TILE - cap
    rows = GROUP * TILE
    bf16 = jnp.bfloat16

    def shift(k):
        i = k // pairs
        de = (eps // 2 + ((i + 1) // 2) * (2 * ((i + 1) % 2) - 1) + eps) % eps
        return (k + 1) % pairs, de

    def target(k):
        dp, de = shift(k)
        return lax.rem(pair + dp, pairs), lax.rem(ep + de, eps)

    def origin(k):
        dp, de = shift(k)
        return lax.rem(pair + pairs - dp, pairs), lax.rem(ep + eps - de, eps)

    tok_load = pltpu.make_async_copy(tok_hbm, tok, tok_sem.at[0])
    tok_load.start()

    barrier = pltpu.get_barrier_semaphore()

    @pl.loop(0, n - 1)
    def _(k):
        p, e = target(k)
        pl.semaphore_signal(barrier, inc=1, device_id=(p, e), device_id_type=MESH)

    loads = [
        pltpu.make_async_copy(src.at[0], dst, w_sem.at[i])
        for i, (src, dst) in enumerate(((gate_hbm, gate), (up_hbm, up), (down_hbm, down)))
    ]
    for load in loads:
        load.start()

    def outbound(k):
        p, e = target(k)
        return pltpu.make_async_remote_copy(
            src_ref=outgoing.at[k],
            dst_ref=recv.at[k],
            send_sem=send1.at[k],
            recv_sem=recv1.at[k],
            device_id=(p, e),
            device_id_type=MESH,
        )

    def inbound(k):
        p, e = origin(k)
        return pltpu.make_async_remote_copy(
            src_ref=result.at[k],
            dst_ref=returned.at[k],
            send_sem=send2.at[k],
            recv_sem=recv2.at[k],
            device_id=(p, e),
            device_id_type=MESH,
        )

    def row_ids(first, shape, axis):
        at = lax.broadcasted_iota(jnp.int32, shape, axis)
        base = jnp.zeros(shape, jnp.int32)
        for i in range(GROUP):
            p, e = target(first + i)
            base = jnp.where(at // TILE == i, (p * eps + e) * TILE, base)
        return base + at % TILE

    def one_hot(mask):
        return mask.astype(jnp.float32).astype(bf16)

    def pack(first):
        ids = row_ids(first, (rows, tok_rows), 0)
        main = one_hot(row_keys[0:1, :] == ids)
        for j in range(parts):
            cols = pl.ds(j * tail, tail)
            ends = one_hot(row_keys[j + 1:j + 2, :] == ids)
            piece = dot(main, tok[:, cols]) + dot(ends, tok[:, width:])
            outgoing[pl.ds(first, GROUP), :, cols] = piece.astype(bf16).reshape(GROUP, TILE, tail)

    def unpack(first, start):
        ids = row_ids(first, (tok_rows, rows), 1)
        main = one_hot(col_keys[:, 0:1] == ids)
        ends = jnp.zeros((tok_rows, tail), jnp.float32)
        for j in range(parts):
            cols = pl.ds(j * tail, tail)
            piece = returned[pl.ds(first, GROUP), :, cols].reshape(rows, tail)
            head = dot(main, piece).astype(bf16)
            head_ref[:, cols] = head if start else head_ref[:, cols] + head
            ends = ends + dot(one_hot(col_keys[:, j + 1:j + 2] == ids), piece)
        ends = ends.astype(bf16)
        ends_ref[...] = ends if start else ends_ref[...] + ends

    def send(first):
        @pl.loop(0, GROUP)
        def _(i):
            @pl.when(first + i < n - 1)
            def _():
                outbound(first + i).start()

    tok_load.wait()
    pack(0)
    pl.semaphore_wait(barrier, n - 1)
    send(0)

    @pl.loop(1, n // GROUP)
    def _(g):
        pack(g * GROUP)
        send(g * GROUP)

    own = pltpu.make_async_copy(outgoing.at[n - 1], recv.at[n - 1], local_sem.at[0])
    own.start()
    for load in loads:
        load.wait()
    own.wait()

    r = lax.broadcasted_iota(jnp.int32, (rows, rows), 0)
    c = lax.broadcasted_iota(jnp.int32, (rows, rows), 1)
    same = (r // TILE) == (c // TILE)
    r, c = r % TILE, c % TILE

    def spreader(j):
        return one_hot(same & (r // spare == j) & (c == cap + r % spare))

    def folder(j):
        return one_hot(same & (r >= cap) & (c == spare * j + r - cap))

    body_row = (lax.broadcasted_iota(jnp.int32, (rows, 1), 0) % TILE) < cap
    step = 256

    @pl.loop(0, n // GROUP)
    def _(g):
        first = g * GROUP

        @pl.loop(0, GROUP)
        def _(i):
            @pl.when(first + i < n - 1)
            def _():
                outbound(first + i).wait_recv()

        block = recv.at[pl.ds(first, GROUP)]
        total = jnp.zeros((rows, tail), jnp.float32)
        for j in range(parts):
            piece = block[:, :, j * tail:(j + 1) * tail].reshape(rows, tail)
            total = total + dot(spreader(j), piece)
        rest[...] = total.astype(bf16)

        @pl.loop(0, hidden.shape[1] // step)
        def _(f):
            cols = pl.ds(pl.multiple_of(f * step, step), step)
            main = block[...].reshape(rows, width)
            g_out = dot(main, gate[:width, cols]) + dot(rest[...], gate[width:, cols])
            u_out = dot(main, up[:width, cols]) + dot(rest[...], up[width:, cols])
            hidden[:, cols] = (jax.nn.silu(g_out) * u_out).astype(bf16)

        rest[...] = dot(hidden[...], down[:, width:]).astype(bf16)
        for j in range(parts):
            cols = pl.ds(j * tail, tail)
            body = dot(hidden[...], down[:, cols])
            extra = dot(folder(j), rest[...])
            packed = jnp.where(body_row, body, extra).astype(bf16)
            result[pl.ds(first, GROUP), :, cols] = packed.reshape(GROUP, TILE, tail)

        @pl.loop(0, GROUP)
        def _(i):
            @pl.when(first + i < n - 1)
            def _():
                inbound(first + i).start()

    mine = pltpu.make_async_copy(result.at[n - 1], returned.at[n - 1], local_sem.at[1])
    mine.start()
    mine.wait()

    def collect(first):
        @pl.loop(0, GROUP)
        def _(i):
            @pl.when(first + i < n - 1)
            def _():
                inbound(first + i).wait_recv()

    collect(0)
    unpack(0, True)

    @pl.loop(1, n // GROUP)
    def _(g):
        collect(g * GROUP)
        unpack(g * GROUP, False)

    @pl.loop(0, n - 1)
    def _(k):
        outbound(k).wait_send()
        inbound(k).wait_send()


def fused(tokens, routed, slot, w_gate, w_up, w_down, pairs, eps, cap):
    n = pairs * eps
    tok_rows, depth = tokens.shape
    ff = w_gate.shape[2]
    spare = TILE - cap
    parts = cap // spare
    tail = depth * spare // TILE
    width = depth - tail

    rest_key = jnp.where(
        slot[None, :] // spare == jnp.arange(parts)[:, None],
        (routed * TILE + cap + slot % spare)[None, :],
        -1,
    )
    keys = jnp.concatenate([(routed * TILE + slot)[None, :], rest_key], axis=0)

    vmem = pl.BlockSpec(memory_space=pltpu.VMEM)
    hbm = pl.BlockSpec(memory_space=pl.ANY)
    bf16 = jnp.bfloat16
    parcels = pltpu.VMEM((n, TILE, width), bf16)
    head, ends = pl.pallas_call(
        functools.partial(exchange_ffn, pairs, eps, cap),
        out_shape=[
            jax.ShapeDtypeStruct((tok_rows, width), bf16),
            jax.ShapeDtypeStruct((tok_rows, tail), bf16),
        ],
        in_specs=[vmem, vmem, hbm, hbm, hbm, hbm],
        out_specs=[vmem, vmem],
        scratch_shapes=[
            pltpu.VMEM((tok_rows, depth), bf16),
            parcels,
            parcels,
            parcels,
            parcels,
            pltpu.VMEM((depth, ff), bf16),
            pltpu.VMEM((depth, ff), bf16),
            pltpu.VMEM((ff, depth), bf16),
            pltpu.VMEM((GROUP * TILE, ff), bf16),
            pltpu.VMEM((GROUP * TILE, tail), bf16),
            pltpu.SemaphoreType.DMA((1,)),
            pltpu.SemaphoreType.DMA((3,)),
            pltpu.SemaphoreType.DMA((2,)),
            pltpu.SemaphoreType.DMA((n,)),
            pltpu.SemaphoreType.DMA((n,)),
            pltpu.SemaphoreType.DMA((n,)),
            pltpu.SemaphoreType.DMA((n,)),
        ],
        compiler_params=pltpu.CompilerParams(
            collective_id=0, has_side_effects=True, vmem_limit_bytes=56 * 1024 * 1024
        ),
        name="exchange_ffn",
    )(keys, keys.T, tokens, w_gate, w_up, w_down)
    return jnp.concatenate([head, ends], axis=1)


def plain(tokens, routed, slot, w_gate, w_up, w_down, experts, capacity):
    position = routed * capacity + slot
    outgoing = (
        jnp.zeros((experts * capacity, tokens.shape[1]), jnp.bfloat16).at[position].set(tokens)
    )
    parcel = lax.all_to_all(
        outgoing.reshape(experts, capacity, outgoing.shape[1]),
        ("pair", "ep"), split_axis=0, concat_axis=0, tiled=True,
    )
    flat_rows = parcel.reshape(experts * capacity, parcel.shape[2])
    gate_proj = dot(flat_rows, w_gate[0])
    up_proj = dot(flat_rows, w_up[0])
    hidden = (jax.nn.silu(gate_proj) * up_proj).astype(jnp.bfloat16)
    result = dot(hidden, w_down[0]).astype(jnp.bfloat16)
    returned = lax.all_to_all(
        result.reshape(experts, capacity, result.shape[1]),
        ("pair", "ep"), split_axis=0, concat_axis=0, tiled=True,
    )
    return jnp.take(returned.reshape(experts * capacity, -1), position, axis=0)


BLOCK = 8


def near_ffn(
    pairs, eps, spill, keys_hbm, tok_hbm, gate_hbm, up_hbm, down_hbm, total, flag_hbm,
    tok, send_b, recv_b, res_b, ret_b, send_x, recv_x, res_x, ret_x, send_s, recv_s, res_s, ret_s,
    keys_ref, note, opinion, verdict, notes, gate, up, down, rows_x, hidden,
    load_sem, w_sem, ssem, rsem,
):
    n = pairs * eps
    near = n // 2
    line = eps // 2
    pair, ep = lax.axis_index("pair"), lax.axis_index("ep")
    rows_y = line // 2
    quarter = near // 2
    side = ep // line
    spot = lax.rem(ep % line + rows_y * (1 - side), line)
    outer, row_y = spot // rows_y, spot % rows_y
    tok_rows, depth = tok.shape
    mid = depth // 2
    ff = hidden.shape[1]
    extra = BLOCK // 2
    bf16, f32, i32 = jnp.bfloat16, jnp.float32, jnp.int32
    none = -4 * n * TILE
    wide = 512

    def peer(k, sign):
        i = k % near
        m = (i % quarter + 1) % quarter
        p = lax.rem(pair + pairs + sign * (m % pairs), pairs)
        y = lax.rem(row_y + rows_y + sign * (m // pairs), rows_y)
        there = lax.rem(side + 1 - k // near, 2)
        plane = lax.rem(outer + 1 - i // quarter + 1 - there, 2)
        return p, there * line + plane * rows_y + y

    barrier = pltpu.get_barrier_semaphore()
    for k in range(n - 1):
        pl.semaphore_signal(barrier, inc=1, device_id=peer(k, 1), device_id_type=MESH)

    key_load = pltpu.make_async_copy(keys_hbm, keys_ref, load_sem.at[0])
    key_load.start()
    tok_load = pltpu.make_async_copy(tok_hbm, tok, load_sem.at[1])
    tok_load.start()

    loads = [
        pltpu.make_async_copy(src.at[0], dst, w_sem.at[i])
        for i, (src, dst) in enumerate(((gate_hbm, gate), (up_hbm, up), (down_hbm, down)))
    ]

    groups = {
        "far": (send_b, recv_b, 0, quarter),
        "far_too": (send_b, recv_b, quarter, near),
        "close": (send_b, recv_b, near, n - 1),
        "extra": (send_x, recv_x, 0, near - 1),
        "spill": (send_s, recv_s, 0, spill),
        "back_far": (res_b, ret_b, 0, quarter),
        "back_far_too": (res_b, ret_b, quarter, near),
        "back_close": (res_b, ret_b, near, n - 1),
        "back_extra": (res_x, ret_x, 0, near - 1),
        "back_spill": (res_s, ret_s, 0, spill),
    }
    ports = {name: i for i, name in enumerate(groups)}

    def remote(at, src, dst, to):
        return pltpu.make_async_remote_copy(
            src_ref=src, dst_ref=dst, send_sem=ssem.at[at], recv_sem=rsem.at[at],
            device_id=to, device_id_type=MESH,
        )

    mirror = peer(near - 1, 1)

    def go(name, turn=0):
        src, dst, low, high = groups[name]
        if src.shape[0] == spill:
            remote(ports[name], src, dst, mirror).start()
            return
        sign = -1 if name[:4] == "back" else 1
        skip = near if src.shape[0] == near else 0

        @pl.loop(0, high - low)
        def _(i):
            k = low + i + turn * quarter
            remote(ports[name] + turn, src.at[k], dst.at[k], peer(k + skip, sign)).start()

    def group(name, turn=0):
        src, dst, low, high = groups[name]
        part = pl.ds(low + turn * quarter, high - low)
        return remote(ports[name] + turn, src.at[part], dst.at[part], mirror)

    inner = 1 - outer
    last = len(groups)
    late = {"back_far": last + 2, "back_spill": last + 3}

    def lanes(j):
        return pl.ds(j * (mid // 2), mid // 2)

    def go_half(name, j):
        src, dst, low, high = groups[name]
        at = late[name] if j else ports[name]
        if src.shape[0] == spill:
            remote(at, src.at[:, :, lanes(j)], dst.at[:, :, lanes(j)], mirror).start()
            return

        @pl.loop(low, high)
        def _(k):
            remote(at, src.at[k, :, lanes(j)], dst.at[k, :, lanes(j)], peer(k, -1)).start()

    def half_group(name, j):
        src, dst, low, high = groups[name]
        part = pl.ds(low, high - low)
        at = late[name] if j else ports[name]
        return remote(at, src.at[part, :, lanes(j)], dst.at[part, :, lanes(j)], mirror)

    tell = remote(last, note, notes.at[near], mirror)

    def vote(k):
        return remote(last + 1, opinion, notes.at[k], peer(k + near, 1))

    votes = remote(last + 1, notes.at[pl.ds(0, near - 1)], notes.at[pl.ds(0, near - 1)], mirror)

    def iota(shape, axis):
        return lax.broadcasted_iota(i32, shape, axis)

    def one_hot(mask):
        return jnp.where(mask, 1.0, 0.0).astype(bf16)

    expert = iota((n, 128), 0)
    order = jnp.zeros((n, 128), i32)
    for k in range(n):
        p, e = peer(k, 1) if k < n - 1 else (pair, ep)
        order = jnp.where(expert == p * eps + e, k, order)
    order = order.astype(f32)
    key_load.wait()
    routed = keys_ref[...]
    which = iota((n, tok_rows), 0)
    chosen = jnp.where(which == routed, 1.0, 0.0)
    earlier = one_hot(iota((tok_rows, tok_rows), 0) < iota((tok_rows, tok_rows), 1))
    before = dot(chosen.astype(bf16), earlier)
    load_of = jnp.sum(chosen, axis=1, keepdims=True)
    over = jnp.where(order < near, jnp.maximum(load_of - BLOCK, 0.0), 0.0)
    ahead = jnp.where(which < routed, over[:, 0:1], 0.0)
    first = jnp.sum(ahead, axis=0, keepdims=True).astype(i32)
    rank = jnp.sum(chosen * order[:, 0:1], axis=0, keepdims=True).astype(i32)
    slot = jnp.sum(chosen * before, axis=0, keepdims=True).astype(i32)
    far = rank < near
    direct = slot < BLOCK
    spot_s = first + slot - BLOCK
    spilled = far & (slot >= BLOCK)
    spill_key = jnp.where(spilled, spot_s, none)

    def split(at, chunk):
        return pl.ds(pl.multiple_of(at + chunk * wide, wide), wide)

    def weave(left, right, count):
        left = left.reshape(count, BLOCK, wide)
        right = right.reshape(count, BLOCK, wide)
        return jnp.concatenate([left, right], axis=1).astype(bf16)

    tok_load.wait()
    for load in loads:
        load.start()

    spill_hot = one_hot(spill_key == iota((spill * BLOCK, tok_rows), 0))

    @pl.loop(0, mid // wide)
    def _(c):
        left = dot(spill_hot, tok[:, split(0, c)])
        right = dot(spill_hot, tok[:, split(mid, c)])
        send_s[:, :, split(0, c)] = weave(left, right, spill)

    pl.semaphore_wait(barrier, n - 1)
    go("spill")

    far_key = jnp.where(far & direct, rank * BLOCK + slot, none)
    beyond = jnp.where(direct, slot, near * BLOCK + slot - BLOCK)
    close_key = jnp.where(far, none, (rank - near) * BLOCK + beyond)
    pack_b = jnp.where(direct, rank * TILE + slot, none)
    pack_x = jnp.where(direct | far, none, (rank - near) * TILE + slot - BLOCK)
    pack_s = jnp.where(spilled, spot_s // BLOCK * TILE + spot_s % BLOCK, none)
    home = rank * TILE + extra + slot - BLOCK + 1
    lines = jnp.concatenate([pack_b, pack_x, pack_s, home, pack_b, pack_b, pack_b, pack_b], axis=0)
    cols = jnp.transpose(lines.astype(f32)).astype(i32)
    col_b, col_x, col_s, col_h = (cols[:, i:i + 1] for i in range(4))
    lane = iota((tok_rows, 128), 1)
    codes = jnp.where(col_s == lane, col_h, 0) + jnp.where(col_s + BLOCK == lane, col_h + BLOCK, 0)
    codes = jnp.sum(codes.astype(f32), axis=0, keepdims=True)
    excess = jnp.sum(over[:, 0:1], axis=0, keepdims=True) > spill * BLOCK
    excess = jnp.where(excess, 1.0, 0.0)
    note[...] = jnp.where(iota((1, 128), 1) == 127, excess, codes)

    tell.start()
    far_hot = one_hot(far_key == iota((near * BLOCK, tok_rows), 0))

    @pl.loop(0, mid // wide)
    def _(c):
        left = dot(far_hot, tok[:, split(0, c)])
        right = dot(far_hot, tok[:, split(mid, c)])
        send_b[pl.ds(0, near), :, split(0, c)] = weave(left, right, near)

    close_hot = one_hot(close_key == iota((2 * near * BLOCK, tok_rows), 0))

    @pl.loop(0, mid // wide)
    def _(c):
        left = dot(close_hot, tok[:, split(0, c)])
        right = dot(close_hot, tok[:, split(mid, c)])
        body = near * BLOCK
        send_b[pl.ds(near, near), :, split(0, c)] = weave(left[:body], right[:body], near)
        send_x[:, :, split(0, c)] = weave(left[body:], right[body:], near)

    @pl.when(inner == 1)
    def _():
        go("far", inner)

    go("close")

    @pl.when(inner == 1)
    def _():
        go("far", outer)

    recv_b[n - 1] = send_b[n - 1]

    tell.wait_recv()
    group("spill").wait_recv()
    code = notes[near]
    depth_s = spill * TILE
    placed = code[:, :depth_s].astype(i32) - 1
    place_hot = one_hot(placed == iota((near * TILE, depth_s), 0))

    @pl.loop(0, mid // wide)
    def _(c):
        moved = dot(place_hot, recv_s[:, :, split(0, c)].reshape(depth_s, wide))
        mine = send_x[:, :, split(0, c)].reshape(near * TILE, wide).astype(f32)
        send_x[:, :, split(0, c)] = (mine + moved).astype(bf16).reshape(near, TILE, wide)

    go("extra")

    @pl.when(outer == 1)
    def _():
        go("far", inner)
        go("far", outer)

    recv_x[near - 1] = send_x[near - 1]

    opinion[...] = jnp.maximum(note[...], code)

    @pl.loop(0, near - 1)
    def _(k):
        vote(k).start()

    diagonal = iota((depth_s, 128), 0) == iota((depth_s, 128), 1)
    wanted = jnp.sum(jnp.where(diagonal, code, 0.0), axis=1, keepdims=True).astype(i32) - 1
    fetch_hot = one_hot(wanted == iota((depth_s, near * TILE), 1))

    for load in loads:
        load.wait()

    def ffn(arrived, result, base, count):
        rows = count * BLOCK

        @pl.loop(0, mid // wide)
        def _(c):
            piece = arrived[pl.ds(base, count), :, split(0, c)].astype(f32)
            rows_x[:rows, split(0, c)] = piece[:, :BLOCK].reshape(rows, wide).astype(bf16)
            rows_x[:rows, split(mid, c)] = piece[:, BLOCK:].reshape(rows, wide).astype(bf16)

        step = 256

        @pl.loop(0, ff // step)
        def _(f):
            at = pl.ds(pl.multiple_of(f * step, step), step)
            g_out = dot(rows_x[:rows, :], gate[:, at])
            u_out = dot(rows_x[:rows, :], up[:, at])
            hidden[:rows, at] = (jax.nn.silu(g_out) * u_out).astype(bf16)

        @pl.loop(0, mid // wide)
        def _(c):
            left = dot(hidden[:rows, :], down[:, split(0, c)])
            right = dot(hidden[:rows, :], down[:, split(mid, c)])
            result[pl.ds(base, count), :, split(0, c)] = weave(left, right, count)

    def unpack(col, returned, base, count, start, part=None):
        depth_k = count * TILE
        at = iota((tok_rows, depth_k), 1) + base * TILE
        left_hot = one_hot(col == at)
        right_hot = one_hot(col + BLOCK == at)
        chunks = mid // wide
        low, high = (0, chunks) if part is None else (part * chunks // 2, (part + 1) * chunks // 2)

        @pl.loop(low, high)
        def _(c):
            piece = returned[pl.ds(base, count), :, split(0, c)].reshape(depth_k, wide)
            for hot, half in ((left_hot, 0), (right_hot, mid)):
                got = dot(hot, piece).astype(bf16)
                total[:, split(half, c)] = got if start else total[:, split(half, c)] + got

    group("close").wait_recv()
    ffn(recv_b, res_b, near, near)
    go("back_close")
    ret_b[n - 1] = res_b[n - 1]
    group("extra").wait_recv()
    ffn(recv_x, res_x, 0, near)
    go("back_extra")
    ret_x[near - 1] = res_x[near - 1]
    for turn in (1, 0):
        group("far", turn).wait_recv()
        ffn(recv_b, res_b, turn * quarter, quarter)
        if turn:
            go("back_far", turn)
        else:
            go_half("back_far", 0)
            go_half("back_far", 1)

    for name in ("spill", "far", "far_too", "close", "extra"):
        group(name).wait_send()
    tell.wait_send()
    votes.wait_send()
    votes.wait_recv()
    worst = jnp.maximum(jnp.max(notes[pl.ds(0, near - 1)], axis=0), opinion[...])
    worst = jnp.where(iota((1, 128), 1) == 127, worst, 0.0)
    verdict[...] = jnp.max(worst, axis=1, keepdims=True)
    report = pltpu.make_async_copy(verdict, flag_hbm, load_sem.at[0])
    report.start()
    group("back_extra").wait_recv()

    @pl.loop(0, mid // wide)
    def _(c):
        piece = ret_x[:, :, split(0, c)].reshape(near * TILE, wide)
        res_s[:, :, split(0, c)] = dot(fetch_hot, piece).astype(bf16).reshape(spill, TILE, wide)

    go_half("back_spill", 0)
    go_half("back_spill", 1)
    unpack(col_x, ret_x, 0, near, True)
    group("back_close").wait_recv()
    unpack(col_b, ret_b, near, near, False)
    def relayed(when):
        @pl.when(outer == when)
        def _():
            for j in range(2):
                half_group("back_spill", j).wait_recv()
                unpack(col_s, ret_s, 0, spill, False, j)

    relayed(1)
    group("back_far", 1).wait_recv()
    unpack(col_b, ret_b, quarter, quarter, False)
    for j in range(2):
        half_group("back_far", j).wait_recv()
        unpack(col_b, ret_b, 0, quarter, False, j)
    relayed(0)
    for name in ("back_close", "back_far_too", "back_extra"):
        group(name).wait_send()
    for j in range(2):
        half_group("back_far", j).wait_send()
        half_group("back_spill", j).wait_send()
    report.wait()


def spilling(tokens, routed, w_gate, w_up, w_down, pairs, eps):
    n = pairs * eps
    near = n // 2
    tok_rows, depth = tokens.shape
    ff = w_gate.shape[2]
    spill = 3
    bf16, f32 = jnp.bfloat16, jnp.float32
    vmem = pl.BlockSpec(memory_space=pltpu.VMEM)
    hbm = pl.BlockSpec(memory_space=pl.ANY)
    dma = pltpu.SemaphoreType.DMA

    def blocks(count):
        return pltpu.VMEM((count, TILE, depth // 2), bf16)

    return pl.pallas_call(
        functools.partial(near_ffn, pairs, eps, spill),
        out_shape=[
            jax.ShapeDtypeStruct((tok_rows, depth), bf16),
            jax.ShapeDtypeStruct((1, 1), f32),
        ],
        in_specs=[hbm, hbm, hbm, hbm, hbm],
        out_specs=[vmem, hbm],
        scratch_shapes=[
            pltpu.VMEM((tok_rows, depth), bf16),
            *[blocks(n)] * 4,
            *[blocks(near)] * 4,
            *[blocks(spill)] * 4,
            pltpu.VMEM((1, tok_rows), jnp.int32),
            pltpu.VMEM((1, 128), f32),
            pltpu.VMEM((1, 128), f32),
            pltpu.VMEM((1, 1), f32),
            pltpu.VMEM((near + 1, 1, 128), f32),
            pltpu.VMEM((depth, ff), bf16),
            pltpu.VMEM((depth, ff), bf16),
            pltpu.VMEM((ff, depth), bf16),
            pltpu.VMEM((near * BLOCK, depth), bf16),
            pltpu.VMEM((near * BLOCK, ff), bf16),
            dma((2,)), dma((3,)), dma((14,)), dma((14,)),
        ],
        compiler_params=pltpu.CompilerParams(
            collective_id=1, has_side_effects=True, vmem_limit_bytes=56 * 1024 * 1024
        ),
        name="near_ffn",
    )(routed.reshape(1, tok_rows), tokens, w_gate, w_up, w_down)


def dispatch(tokens, routed, w_gate, w_up, w_down, pairs, eps):
    experts = pairs * eps
    tok_rows, depth = tokens.shape
    cap = tok_rows // experts + tok_rows // (2 * experts)
    onehot = (routed[:, None] == jnp.arange(experts, dtype=jnp.int32)[None, :]).astype(jnp.float32)
    order = jnp.arange(tok_rows)
    earlier = (order[:, None] > order[None, :]).astype(jnp.bfloat16)
    before = dot(earlier, onehot.astype(jnp.bfloat16))
    slot = jnp.sum(before * onehot, axis=1).astype(jnp.int32)
    spare = TILE - cap
    packs = 0 < spare <= cap and cap % spare == 0 and (depth * spare) % (TILE * 256) == 0
    if packs and experts % GROUP == 0 and w_gate.shape[2] % 256 == 0:
        return fused(tokens, routed, slot, w_gate, w_up, w_down, pairs, eps, cap)
    return plain(tokens, routed, slot, w_gate, w_up, w_down, experts, cap)


def shards(tokens, expert_of, w_gate, w_up, w_down):
    pairs = lax.axis_size("pair")
    eps = lax.axis_size("ep")
    experts = pairs * eps
    tok_rows, depth = tokens.shape
    routed = expert_of[:, 0]
    whole = (tokens, routed, w_gate, w_up, w_down)
    even = tok_rows == BLOCK * experts and eps % 4 == 0 and experts % (2 * GROUP) == 0
    if not (even and depth % 1024 == 0 and w_gate.shape[2] % 256 == 0):
        return dispatch(*whole, pairs, eps)
    result, flag = spilling(*whole, pairs, eps)
    return lax.cond(
        flag[0, 0] > 0,
        lambda: dispatch(*whole, pairs, eps),
        lambda: result,
    )


def solution(mesh):
    spec2 = P(("pair", "ep"), None)
    spec3 = P(("pair", "ep"), None, None)
    return jax.shard_map(
        shards,
        mesh=mesh,
        in_specs=(spec2, spec2, spec3, spec3, spec3),
        out_specs=spec2,
        check_vma=False,
    )
```
